256 devices in a mesh: orb: 64 (over x, z, core), rep: 4 (over y).
Axes of the slice: x: 4, y: 4, z: 8, core: 2. Of those that a mesh axis runs over, the one named last changes fastest.
Arguments:
- orbitals: float32 [128, 64, 4096], P('orb'), may hold values from -6 to 6
- pair_list: int32 [1024, 3], P(('orb', 'rep')), may hold values from 0 to 127, as said below
- box_offsets: int32 [128, 3], replicated, may hold values from 0 to 1023, as said below
Outputs:
- exchange_forces: float32 [128, 64, 4096], P('orb')
- slab_field: float32 [1024, 9216], P('orb')
The draws below stay inside these ranges and needn't reach their ends.
Inputs may be any that keep to these rules, and one draw needn't show every extreme that they name: `pair_list`: the rows of one device are the 4 slots of block d, blocks in order of orb then rep. Their first orbital belongs to orbital group g = d // 4 (numbers g * 2 to g * 2 + 1); their second belongs to group g - 1, g or g + 1. The live flag is 1 on the first 1 to 4 rows of each block and 0 after; in every draw some block is all live. `box_offsets`: orbital k's z offset lies from (k // 2) * 16 to that plus 16 - 1; its x and y offsets lie from 0 to 31.
All inputs are finite; a program needn't handle non-finite values.
Results may differ from the reference program's by a relative error of at most 0.0003.
Values sent between devices are 32-bit elements; how exact they have to be, the bound alone decides.
No kernel may reach another device: no remote copies, remote signals or barrier semaphores. Data moves between devices by JAX's collectives and lax.ppermute only.
A program may use at most 128 MiB of HBM per device.

```python
import jax
import jax.numpy as jnp
from jax import lax

BOX = 64
SLAB = 16
WIDE = 96
ORB_DEV = 2
PAIR_DEV = 4
ITERS = 5
ORBITALS = 128
PAIRS = 1024
NZ = 1024
N_ORB = 64
N_REP = 4


def draw_box_offsets(key, part):
    key_depth = jax.random.fold_in(key, 11)
    key_plane = jax.random.fold_in(key, 12)
    group = jnp.arange(ORBITALS, dtype=jnp.int32) // ORB_DEV
    depth = group * SLAB + jax.random.randint(key_depth, (ORBITALS,), 0, SLAB)
    plane = jax.random.randint(key_plane, (ORBITALS, 2), 0, WIDE - BOX)
    return jnp.concatenate([depth[:, None], plane], axis=1).astype(jnp.int32)


def draw_pair_list(key, part):
    rows = jnp.arange(PAIRS, dtype=jnp.int32)
    block = rows // PAIR_DEV
    place = rows % PAIR_DEV
    group = block // N_REP
    blocks = PAIRS // PAIR_DEV
    first = group * ORB_DEV + jax.random.randint(jax.random.fold_in(key, 21), (PAIRS,), 0, ORB_DEV)
    other = jnp.clip(group + jax.random.randint(jax.random.fold_in(key, 22), (PAIRS,), -1, 2), 0, N_ORB - 1)
    second = other * ORB_DEV + jax.random.randint(jax.random.fold_in(key, 23), (PAIRS,), 0, ORB_DEV)
    low_one = jax.random.randint(jax.random.fold_in(key, 24), (blocks,), 0, PAIR_DEV)
    low_two = jax.random.randint(jax.random.fold_in(key, 25), (blocks,), 0, PAIR_DEV)
    filled = jax.random.randint(jax.random.fold_in(key, 26), (), 0, blocks)
    counts = jnp.where(jnp.arange(blocks, dtype=jnp.int32) == filled, PAIR_DEV, jnp.minimum(low_one, low_two) + 1)
    live = (place < counts[block]).astype(jnp.int32)
    return jnp.stack([first, second, live], axis=1).astype(jnp.int32)


def shard_levels(rng, dims, pieces, least, top_value):
    factor_of, own = 1.0, jax.random.fold_in(rng, 6)
    for dim, blocks in pieces:
        draws = jnp.exp(jax.random.uniform(jax.random.fold_in(own, dim), (blocks,), jnp.float32, least / len(pieces), top_value / len(pieces)))
        factor_of = factor_of * jnp.repeat(draws, dims[dim] // blocks).reshape([-1 if axis == dim else 1 for axis in range(len(dims))])
    return factor_of


def noise(own_key, shape, deviation, most, cuts=(), kind=jnp.bfloat16):
    result = jax.random.normal(own_key, shape, jnp.float32) * deviation
    if len(cuts) > 0:
        result = shard_levels(own_key, shape, cuts, -0.22, 0.18) * result
    return jnp.clip(result, min=-most, max=most).astype(kind)


def setup_inputs(seed: int = 0) -> dict:
    key_list = jax.random.split(jax.random.key(seed), 4)
    orbitals = noise(key_list[0], (ORBITALS, BOX, BOX * BOX), 1.0, 6.0, ((0, 64),), jnp.float32)
    pair_list = draw_pair_list(jax.random.fold_in(key_list[3], 71), 0)
    box_offsets = draw_box_offsets(jax.random.fold_in(key_list[3], 71), 0)
    return {"orbitals": orbitals, "pair_list": pair_list, "box_offsets": box_offsets}


SCREEN = 6.1


def move_box(box, dz, dx, dy):
    side = box.shape[0]
    rows = jnp.arange(side, dtype=jnp.int32)
    flat = jnp.arange(side * side, dtype=jnp.int32)
    xpos = flat // side
    ypos = flat % side
    rolled = jnp.roll(box, dz, axis=0)
    rolled = jnp.roll(rolled, dx * side + dy, axis=1)
    zgood = (rows - dz >= 0) & (rows - dz < side)
    cgood = (xpos - dx >= 0) & (xpos - dx < side) & (ypos - dy >= 0) & (ypos - dy < side)
    return jnp.where(zgood[:, None] & cgood[None, :], rolled, jnp.zeros_like(rolled))


def operate(field):
    side = field.shape[0]
    ypos = jnp.arange(side * side, dtype=jnp.int32) % side
    zpad = jnp.pad(field, ((1, 1), (0, 0)))
    beside = zpad[2:] + zpad[:-2]
    cpad = jnp.pad(field, ((0, 0), (side, side)))
    beside = beside + cpad[:, 2 * side:] + cpad[:, :-2 * side]
    upper = cpad[:, side + 1:side + 1 + side * side]
    lower = cpad[:, side - 1:side - 1 + side * side]
    beside = beside + jnp.where(ypos < side - 1, upper, 0.0) + jnp.where(ypos > 0, lower, 0.0)
    return SCREEN * field - beside


def solve(density):
    potential = jnp.zeros_like(density)
    residual = density
    direction = density
    norm_now = jnp.sum(residual * residual)
    for step in range(ITERS):
        image = operate(direction)
        alpha = norm_now / jnp.sum(direction * image)
        potential = potential + alpha * direction
        residual = residual - alpha * image
        norm_next = jnp.sum(residual * residual)
        direction = residual + (norm_next / norm_now) * direction
        norm_now = norm_next
    return potential


def place_box(box, offx, offy):
    side = box.shape[0]
    cube = box.reshape(side, side, side)
    cube = jnp.pad(cube, ((0, 0), (0, 0), (0, WIDE - side)))
    cube = jnp.roll(cube, offy, axis=2).reshape(side, side * WIDE)
    sheet = jnp.pad(cube, ((0, 0), (0, WIDE * WIDE - side * WIDE)))
    return jnp.roll(sheet, offx * WIDE, axis=1)


def reference(orbitals, pair_list, box_offsets):
    def one_pair(t, forces):
        first = pair_list[t, 0]
        second = pair_list[t, 1]
        delta = box_offsets[first] - box_offsets[second]

        def work(acc):
            shifted = move_box(orbitals[first], delta[0], delta[1], delta[2])
            potential = solve(orbitals[second] * shifted)
            acc = acc.at[second].add(potential * shifted)
            back = move_box(potential * orbitals[second], -delta[0], -delta[1], -delta[2])
            return acc.at[first].add(back)

        return lax.cond(pair_list[t, 2] > 0, work, lambda acc: acc, forces)

    forces = lax.fori_loop(0, PAIRS, one_pair, jnp.zeros_like(orbitals))

    def deposit(k, field):
        sheet = place_box(forces[k], box_offsets[k, 1], box_offsets[k, 2])
        rows = (box_offsets[k, 0] + jnp.arange(BOX, dtype=jnp.int32)) % NZ
        return field.at[rows].add(sheet)

    field = lax.fori_loop(0, ORBITALS, deposit, jnp.zeros((NZ, WIDE * WIDE), orbitals.dtype))
    return forces, field
```

```python
import functools

import jax
import jax.numpy as jnp
from jax import lax
from jax.experimental import pallas as pl
from jax.experimental.pallas import tpu as pltpu
from jax.sharding import PartitionSpec as P

BOX = 64
SLAB = 16
WIDE = 96
ITERS = 5
SCREEN = 6.1
LANES = 128
COLS = BOX * BOX // LANES
FRONT = 16
ROOM = 32
VMEM_LIMIT = 60 * 1024 * 1024


def lane_of(rows):
    return lax.broadcasted_iota(jnp.int32, (rows, LANES), 1)


def fold(block):
    return jnp.sum(block.reshape(BOX // 8, 8, LANES), axis=0)


def total(partial):
    return jnp.sum(jnp.sum(partial, axis=1, keepdims=True), axis=0, keepdims=True)


def shift_reader(buffer, dz, dx, dy):
    lanes = lane_of(BOX)
    flat = dx * BOX + dy
    blocks = flat >> 7
    turn = flat & (LANES - 1)
    ypos = lanes & (BOX - 1)
    inside = (ypos >= dy) & (ypos < BOX + dy)
    early = lanes < LANES - turn

    def read(c):
        near = buffer[c - blocks + FRONT, pl.ds(ROOM - dz, BOX), :]
        before = buffer[c - blocks + FRONT - 1, pl.ds(ROOM - dz, BOX), :]
        turned = pltpu.roll(jnp.where(early, near, before), turn, 1)
        return jnp.where(inside, turned, 0.0)

    return read


def beside(field, c, center, after):
    lanes = lane_of(BOX)
    ypos = lanes & (BOX - 1)
    above = field[c + 1, pl.ds(9, BOX), :]
    below = field[c + 1, pl.ds(7, BOX), :]
    ahead = field[c, pl.ds(8, BOX), :]
    across = pltpu.roll(center + jnp.where(lanes < BOX, after, ahead), BOX, 1)
    left = jnp.where(ypos > 0, pltpu.roll(center, 1, 1), 0.0)
    right = jnp.where(ypos < BOX - 1, pltpu.roll(center, LANES - 1, 1), 0.0)
    return (across + (above + below)) + (left + right)


def solve_pair(stage, first, second, delta, buffer, shifted, basis, image):
    def load_first(c, carry):
        buffer[c + FRONT, pl.ds(ROOM, BOX), :] = stage[first, :, pl.ds(pl.multiple_of(c * LANES, LANES), LANES)]
        return carry

    lax.fori_loop(0, COLS, load_first, 0, unroll=4)
    read = shift_reader(buffer, *delta)
    diagonal, coupling = [], []
    norm_before = None
    for k in range(ITERS):
        field = basis.at[k]

        def value_of(c):
            if k == 0:
                moved = read(c)
                shifted[c] = moved
                return stage[second, :, pl.ds(pl.multiple_of(c * LANES, LANES), LANES)] * moved
            fresh = image[c] - diagonal[k - 1] * basis[k - 1, c + 1, pl.ds(8, BOX), :]
            if k > 1:
                fresh = fresh - coupling[k - 1] * basis[k - 2, c + 1, pl.ds(8, BOX), :]
            return fresh

        def apply(c, center, after, cross):
            result = beside(field, c, center, after)
            if k < ITERS - 1:
                image[c] = result
            return cross + fold(center * result)

        opening = value_of(0)
        field[1, pl.ds(8, BOX), :] = opening
        zero = jnp.zeros((8, LANES), jnp.float32)

        def step(c, carry):
            norm, cross = carry
            after = value_of(c)
            field[c + 1, pl.ds(8, BOX), :] = after
            center = field[c, pl.ds(8, BOX), :]
            cross = apply(c - 1, center, after, cross)
            return norm + fold(after * after), cross

        norm, cross = lax.fori_loop(1, COLS, step, (fold(opening * opening), zero))
        last = field[COLS, pl.ds(8, BOX), :]
        cross = apply(COLS - 1, last, jnp.zeros_like(last), cross)
        norm = total(norm)
        diagonal.append(total(cross) / norm)
        coupling.append(norm / norm_before if k > 0 else None)
        norm_before = norm
    pivots = [SCREEN - diagonal[0]]
    rights = [jnp.ones_like(pivots[0])]
    for k in range(1, ITERS):
        pivots.append(SCREEN - diagonal[k] - coupling[k] / pivots[k - 1])
        rights.append(rights[k - 1] / pivots[k - 1])
    weights = [None] * ITERS
    weights[ITERS - 1] = rights[ITERS - 1] / pivots[ITERS - 1]
    for k in range(ITERS - 2, -1, -1):
        weights[k] = (rights[k] + coupling[k + 1] * weights[k + 1]) / pivots[k]
    return weights


def run_pair(stage, first, second, delta, to_second, to_first, forces, buffer, shifted, basis, image):
    weights = solve_pair(stage, first, second, delta, buffer, shifted, basis, image)

    def finish(c, carry):
        potential = weights[0] * basis[0, c + 1, pl.ds(8, BOX), :]
        for k in range(1, ITERS):
            potential = potential + weights[k] * basis[k, c + 1, pl.ds(8, BOX), :]
        image[c] = potential
        near = stage[second, :, pl.ds(pl.multiple_of(c * LANES, LANES), LANES)]
        buffer[c + FRONT, pl.ds(ROOM, BOX), :] = potential * near
        return carry

    lax.fori_loop(0, COLS, finish, 0)

    @pl.when(to_second)
    def _():
        def deposit(c, carry):
            forces[second, c] = forces[second, c] + image[c] * shifted[c]
            return carry

        lax.fori_loop(0, COLS, deposit, 0, unroll=2)

    @pl.when(to_first)
    def _():
        read = shift_reader(buffer, -delta[0], -delta[1], -delta[2])

        def deposit(c, carry):
            forces[first, c] = forces[first, c] + read(c)
            return carry

        lax.fori_loop(0, COLS, deposit, 0, unroll=2)


def pairs_kernel(begun, *refs):
    if begun:
        info, lists, offsets, own, other, tally, forces_in, forces, tally_out = refs[:9]
    else:
        info, lists, offsets, own, other, forces, tally_out = refs[:7]
    stage, buffer, shifted, basis, image, own_sem, other_sem, force_sem = refs[-8:]
    group, mine, neighbour, which = info[0], info[1], info[2], info[3]
    copies = [
        pltpu.make_async_copy(own, stage.at[pl.ds(0, 2)], own_sem),
        pltpu.make_async_copy(other, stage.at[pl.ds(2, 2)], other_sem),
    ]
    if begun:
        copies.append(pltpu.make_async_copy(forces_in, forces, force_sem))
    for copy in copies:
        copy.start()

    def clear(c, carry):
        buffer[c] = jnp.zeros((BOX + 2 * ROOM, LANES), jnp.float32)
        return carry

    lax.fori_loop(0, COLS + 2 * FRONT, clear, 0)
    nothing = jnp.zeros((BOX + 16, LANES), jnp.float32)
    for k in range(ITERS):
        basis[k, 0] = nothing
        basis[k, COLS + 1] = nothing

        def clear_ends(c, carry):
            basis[k, c + 1, pl.ds(0, 8), :] = jnp.zeros((8, LANES), jnp.float32)
            basis[k, c + 1, pl.ds(BOX + 8, 8), :] = jnp.zeros((8, LANES), jnp.float32)
            return carry

        lax.fori_loop(0, COLS, clear_ends, 0, unroll=4)
    if not begun:

        def clear_forces(c, carry):
            for k in range(2):
                forces[k, c] = jnp.zeros((BOX, LANES), jnp.float32)
            return carry

        lax.fori_loop(0, COLS, clear_forces, 0)
    for copy in copies:
        copy.wait()

    def slot(n, count):
        foreign = n // 16
        row = n % 16
        base = (row // 4) * 36 + foreign * which * 12 + (row % 4) * 3
        first = lists[base]
        second = lists[base + 1]
        live = lists[base + 2] > 0
        second_group = second // 2
        inner = second_group == group
        outer = second_group == neighbour
        if begun:
            wanted = jnp.where(foreign > 0, inner, outer)
        else:
            wanted = jnp.where(foreign > 0, inner, inner | outer)
        taken = live & wanted
        turn = taken & (lax.rem(count, 4) == mine)

        @pl.when(turn)
        def _():
            delta = [offsets[first * 3 + axis] - offsets[second * 3 + axis] for axis in range(3)]
            first_at = jnp.where(foreign > 0, 2 + first - 2 * neighbour, first - 2 * group)
            second_at = jnp.where(inner, second - 2 * group, 2 + second - 2 * neighbour)
            run_pair(
                stage, first_at, second_at, delta, inner, foreign == 0, forces, buffer, shifted, basis, image
            )

        return count + taken.astype(jnp.int32)

    tally_out[0] = lax.fori_loop(0, 32, slot, tally[0] if begun else jnp.int32(0))


def run_pairs(info, lists, offsets, own, other, before=None):
    begun = before is not None
    smem = pl.BlockSpec(memory_space=pltpu.SMEM)
    hbm = pl.BlockSpec(memory_space=pl.ANY)
    vmem = pl.BlockSpec(memory_space=pltpu.VMEM)
    operands = [info, lists, offsets, own, other]
    in_specs = [smem, smem, smem, hbm, hbm]
    if begun:
        operands += [before[1], before[0]]
        in_specs += [smem, hbm]
    return pl.pallas_call(
        functools.partial(pairs_kernel, begun),
        out_shape=(
            jax.ShapeDtypeStruct((2, COLS, BOX, LANES), jnp.float32),
            jax.ShapeDtypeStruct((1,), jnp.int32),
        ),
        in_specs=in_specs,
        out_specs=(vmem, smem),
        scratch_shapes=[
            pltpu.VMEM((4, BOX, BOX * BOX), jnp.float32),
            pltpu.VMEM((COLS + 2 * FRONT, BOX + 2 * ROOM, LANES), jnp.float32),
            pltpu.VMEM((COLS, BOX, LANES), jnp.float32),
            pltpu.VMEM((ITERS, COLS + 2, BOX + 16, LANES), jnp.float32),
            pltpu.VMEM((COLS, BOX, LANES), jnp.float32),
            pltpu.SemaphoreType.DMA,
            pltpu.SemaphoreType.DMA,
            pltpu.SemaphoreType.DMA,
        ],
        compiler_params=pltpu.CompilerParams(vmem_limit_bytes=VMEM_LIMIT),
        cost_estimate=pl.CostEstimate(flops=200_000_000, bytes_accessed=8 << 20, transcendentals=0),
        name="pairs_far" if begun else "pairs_near",
    )(*operands)


def passed_along(block, axis, distance):
    devices = range(lax.axis_size(axis))
    route = [((i - distance) % len(devices), i) for i in devices]
    return lax.ppermute(block, axis, route)


def place_box(box, offx, offy):
    side = box.shape[0]
    cube = box.reshape(side, side, side)
    cube = jnp.pad(cube, ((0, 0), (0, 0), (0, WIDE - side)))
    cube = jnp.roll(cube, offy, axis=2).reshape(side, side * WIDE)
    sheet = jnp.pad(cube, ((0, 0), (0, WIDE * WIDE - side * WIDE)))
    return jnp.roll(sheet, offx * WIDE, axis=1)


def shards(orbitals, pair_list, box_offsets):
    count = orbitals.shape[0]
    group = lax.axis_index("orb")
    groups = lax.axis_size("orb")
    mine = lax.axis_index("rep")
    members = lax.axis_size("rep")
    to_near = [(g, g ^ 1) for g in range(groups)]
    to_far = [(g, g + (1 if g % 2 else -1)) for g in range(groups) if 0 <= g + (1 if g % 2 else -1) < groups]
    slots = pair_list.reshape(-1)
    near_slots = lax.ppermute(slots, "orb", to_near)
    far_slots = lax.ppermute(slots, "orb", to_far)
    near = lax.ppermute(orbitals, "orb", to_near)
    far = lax.ppermute(orbitals, "orb", to_far)
    known = jnp.concatenate([slots, near_slots, far_slots])
    copies = jnp.broadcast_to(known, (members, known.shape[0]))
    lists = lax.all_to_all(copies, "rep", split_axis=0, concat_axis=0, tiled=True).reshape(-1)
    offsets = box_offsets.reshape(-1)
    near_group = group ^ 1
    far_group = group + 2 * (group & 1) - 1
    info = jnp.stack([group, mine, near_group, 1]).astype(jnp.int32)
    before = run_pairs(info, lists, offsets, orbitals, near)
    info = jnp.stack([group, mine, far_group, 2]).astype(jnp.int32)
    partial_forces, _ = run_pairs(info, lists, offsets, orbitals, far, before)
    forces = lax.psum(partial_forces, "rep")
    forces = jnp.swapaxes(forces, 1, 2).reshape(count, BOX, BOX * BOX)
    base = group * count
    window = jnp.zeros((BOX + SLAB, WIDE * WIDE), jnp.float32)
    for orbital in range(count):
        place = box_offsets[base + orbital]
        sheet = place_box(forces[orbital], place[1], place[2])
        depth = place[0] - group * SLAB
        current = lax.dynamic_slice_in_dim(window, depth, BOX, 0)
        window = lax.dynamic_update_slice_in_dim(window, current + sheet, depth, 0)
    slab = window[:SLAB]
    for later in range(1, BOX // SLAB + 1):
        slab = slab + passed_along(window[later * SLAB : (later + 1) * SLAB], "orb", later)
    return (forces, slab)


def solution(mesh):
    in_specs = (P("orb", None, None), P(("orb", "rep"), None), P())
    out_specs = (P("orb", None, None), P("orb", None))
    return jax.shard_map(shards, mesh=mesh, in_specs=in_specs, out_specs=out_specs, check_vma=False)
```

```python
import functools

import jax
import jax.numpy as jnp
import numpy as np
from jax import lax
from jax.experimental import pallas as pl
from jax.experimental.pallas import tpu as pltpu
from jax.sharding import PartitionSpec as P

BOX = 64
SLAB = 16
WIDE = 96
ITERS = 5
SCREEN = 6.1
LANES = 128
COLS = BOX * BOX // LANES
FRONT = 16
GROUP = 16
ROOM = 32
QUARTER = COLS // 4
SLABS = BOX // SLAB + 1
SPAN = WIDE * BOX // 4 + 32 * WIDE
VMEM_LIMIT = 32 * 1024 * 1024
SMEM = pl.BlockSpec(memory_space=pltpu.SMEM)
VMEM = pl.BlockSpec(memory_space=pltpu.VMEM)
HBM = pl.BlockSpec(memory_space=pl.ANY)


def place():
    return lax.axis_index("orb"), lax.axis_index("rep")


def neighbours(group):
    return group ^ 1, group + 2 * (group & 1) - 1


def lane_of(rows):
    return lax.broadcasted_iota(jnp.int32, (rows, LANES), 1)


def fold(block):
    return jnp.sum(block.reshape(BOX // 8, 8, LANES), axis=0)


def total(partial):
    return jnp.sum(jnp.sum(partial, axis=1, keepdims=True), axis=0, keepdims=True)


def shift_reader(buffer, dz, dx, dy):
    lanes = lane_of(BOX)
    flat = dx * BOX + dy
    blocks = flat >> 7
    turn = flat & (LANES - 1)
    ypos = lanes & (BOX - 1)
    inside = (ypos >= dy) & (ypos < BOX + dy)
    early = lanes < LANES - turn

    def read(c):
        near = buffer[c - blocks + FRONT, pl.ds(ROOM - dz, BOX), :]
        before = buffer[c - blocks + FRONT - 1, pl.ds(ROOM - dz, BOX), :]
        turned = pltpu.roll(jnp.where(early, near, before), turn, 1)
        return jnp.where(inside, turned, 0.0)

    return read


def beside(field, c, center, after, within):
    above = field[c + 1, pl.ds(9, BOX), :]
    below = field[c + 1, pl.ds(7, BOX), :]
    ahead = field[c, pl.ds(8, BOX), :]
    across = pltpu.roll(jnp.where(lane_of(BOX) < BOX, after, ahead), BOX, 1)
    high = center.astype(jnp.bfloat16)
    low = (center - high.astype(jnp.float32)).astype(jnp.bfloat16)
    inner = jnp.dot(jnp.concatenate([high, low], axis=1), within[...], preferred_element_type=jnp.float32)
    return (inner + across) + (above + below)


def solve_pair(stage, first, second, delta, within, buffer, shifted, basis, image):
    def load_first(c, carry):
        buffer[c + FRONT, pl.ds(ROOM, BOX), :] = stage[first, :, pl.ds(pl.multiple_of(c * LANES, LANES), LANES)]
        return carry

    lax.fori_loop(0, COLS, load_first, 0, unroll=8)
    read = shift_reader(buffer, *delta)
    diagonal, coupling = [], []
    norm_before = None
    for k in range(ITERS):
        field = basis.at[k]

        def value_of(c):
            if k == 0:
                moved = read(c)
                shifted[c] = moved
                return stage[second, :, pl.ds(pl.multiple_of(c * LANES, LANES), LANES)] * moved
            fresh = image[c] - diagonal[k - 1] * basis[k - 1, c + 1, pl.ds(8, BOX), :]
            if k > 1:
                fresh = fresh - coupling[k - 1] * basis[k - 2, c + 1, pl.ds(8, BOX), :]
            return fresh

        def group(start, carry, final):
            norm, cross = carry
            center = field[start + 1, pl.ds(8, BOX), :]
            values = [center]
            for u in range(1, GROUP + 1):
                if final and u == GROUP:
                    values.append(jnp.zeros_like(center))
                    continue
                fresh = value_of(start + u)
                field[start + u + 1, pl.ds(8, BOX), :] = fresh
                norm = norm + fold(fresh * fresh)
                values.append(fresh)
            for u in range(GROUP):
                result = beside(field, start + u, values[u], values[u + 1], within)
                if k < ITERS - 1:
                    image[start + u] = result
                cross = cross + fold(values[u] * result)
            return norm, cross

        opening = value_of(0)
        field[1, pl.ds(8, BOX), :] = opening
        carry = (fold(opening * opening), jnp.zeros((8, LANES), jnp.float32))
        carry = lax.fori_loop(0, COLS // GROUP - 1, lambda m, held: group(m * GROUP, held, False), carry)
        norm, cross = group(COLS - GROUP, carry, True)
        norm = total(norm)
        diagonal.append(total(cross) / norm)
        coupling.append(norm / norm_before if k > 0 else None)
        norm_before = norm
    pivots = [SCREEN - diagonal[0]]
    rights = [jnp.ones_like(pivots[0])]
    for k in range(1, ITERS):
        pivots.append(SCREEN - diagonal[k] - coupling[k] / pivots[k - 1])
        rights.append(rights[k - 1] / pivots[k - 1])
    weights = [None] * ITERS
    weights[ITERS - 1] = rights[ITERS - 1] / pivots[ITERS - 1]
    for k in range(ITERS - 2, -1, -1):
        weights[k] = (rights[k] + coupling[k + 1] * weights[k + 1]) / pivots[k]
    return weights


def run_pair(stage, first, second, delta, to_second, to_first, within, forces, buffer, shifted, basis, image):
    weights = solve_pair(stage, first, second, delta, within, buffer, shifted, basis, image)

    def finish(c, carry):
        potential = weights[0] * basis[0, c + 1, pl.ds(8, BOX), :]
        for k in range(1, ITERS):
            potential = potential + weights[k] * basis[k, c + 1, pl.ds(8, BOX), :]
        image[c] = potential
        near = stage[second, :, pl.ds(pl.multiple_of(c * LANES, LANES), LANES)]
        buffer[c + FRONT, pl.ds(ROOM, BOX), :] = potential * near
        return carry

    lax.fori_loop(0, COLS, finish, 0, unroll=4)

    @pl.when(to_second)
    def _():
        def deposit(c, carry):
            forces[second, c] = forces[second, c] + image[c] * shifted[c]
            return carry

        lax.fori_loop(0, COLS, deposit, 0, unroll=4)

    @pl.when(to_first)
    def _():
        read = shift_reader(buffer, -delta[0], -delta[1], -delta[2])

        def deposit(c, carry):
            forces[first, c] = forces[first, c] + read(c)
            return carry

        lax.fori_loop(0, COLS, deposit, 0, unroll=8)


def pairs_kernel(begun, *refs):
    if begun:
        lists, offsets, own, other, within, tally, forces_in, *parts, forces, part_sems = refs[:13]
    else:
        lists, offsets, own, other, within, forces, tally_out = refs[:7]
    stage, buffer, shifted, basis, image, own_sem, other_sem, force_sem = refs[-8:]
    group, mine = place()
    near, far = neighbours(group)
    neighbour, which = (far, 2) if begun else (near, 1)
    copies = [
        pltpu.make_async_copy(own, stage.at[pl.ds(0, 2)], own_sem),
        pltpu.make_async_copy(other, stage.at[pl.ds(2, 2)], other_sem),
    ]
    if begun:
        copies.append(pltpu.make_async_copy(forces_in, forces, force_sem))
    for copy in copies:
        copy.start()

    def clear(c, carry):
        buffer[c] = jnp.zeros((BOX + 2 * ROOM, LANES), jnp.float32)
        return carry

    lax.fori_loop(0, COLS + 2 * FRONT, clear, 0, unroll=4)
    nothing = jnp.zeros((BOX + 16, LANES), jnp.float32)
    for k in range(ITERS):
        basis[k, 0] = nothing
        basis[k, COLS + 1] = nothing

        def clear_ends(c, carry):
            basis[k, c + 1, pl.ds(0, 8), :] = jnp.zeros((8, LANES), jnp.float32)
            basis[k, c + 1, pl.ds(BOX + 8, 8), :] = jnp.zeros((8, LANES), jnp.float32)
            return carry

        lax.fori_loop(0, COLS, clear_ends, 0, unroll=4)
    if not begun:

        def clear_forces(c, carry):
            for k in range(2):
                forces[k, c] = jnp.zeros((BOX, LANES), jnp.float32)
            return carry

        lax.fori_loop(0, COLS, clear_forces, 0)
    for copy in copies:
        copy.wait()

    def slot(n, count):
        foreign = n // 16
        row = n % 16
        base = ((row // 4) ^ mine) * 36 + foreign * which * 12 + (row % 4) * 3
        first = lists[base]
        second = lists[base + 1]
        live = lists[base + 2] > 0
        second_group = second // 2
        inner = second_group == group
        outer = second_group == neighbour
        if begun:
            wanted = jnp.where(foreign > 0, inner, outer)
        else:
            wanted = jnp.where(foreign > 0, inner, inner | outer)
        taken = live & wanted
        turn = taken & (lax.rem(count, 4) == mine)

        @pl.when(turn)
        def _():
            delta = [offsets[first * 3 + axis] - offsets[second * 3 + axis] for axis in range(3)]
            first_at = jnp.where(foreign > 0, 2 + first - 2 * neighbour, first - 2 * group)
            second_at = jnp.where(inner, second - 2 * group, 2 + second - 2 * neighbour)
            run_pair(
                stage, first_at, second_at, delta, inner, foreign == 0, within, forces, buffer, shifted, basis, image
            )

        return count + taken.astype(jnp.int32)

    if not begun:
        tally_out[0] = lax.fori_loop(0, 32, slot, jnp.int32(0))
        return
    lax.fori_loop(0, 32, slot, tally[0])
    moves = []
    for k, side in enumerate((1, 3)):
        for n, who in enumerate((mine ^ side, mine)):
            for half, quarter in enumerate((who, who ^ (4 - side))):
                moves.append(
                    pltpu.make_async_copy(
                        forces.at[k, pl.ds(quarter * QUARTER, QUARTER)],
                        parts[2 * k + n].at[pl.ds(half * QUARTER, QUARTER)],
                        part_sems.at[len(moves)],
                    )
                )
    for move in moves:
        move.start()
    for move in moves:
        move.wait()


def within_block():
    lane = np.arange(LANES)
    gap = np.abs(lane[:, None] - lane[None, :])
    same_row = lane[:, None] // BOX == lane[None, :] // BOX
    once = ((gap == 1) & same_row) | (gap == BOX)
    return jnp.asarray(np.concatenate([once, once]), jnp.bfloat16)


def run_pairs(lists, offsets, own, other, before=None):
    begun = before is not None
    operands = [lists, offsets, own, other, within_block()]
    in_specs = [SMEM, SMEM, HBM, HBM, VMEM]
    whole = (2, COLS, BOX, LANES)
    scratch = [
        pltpu.VMEM((4, BOX, BOX * BOX), jnp.float32),
        pltpu.VMEM((COLS + 2 * FRONT, BOX + 2 * ROOM, LANES), jnp.float32),
        pltpu.VMEM((COLS, BOX, LANES), jnp.float32),
        pltpu.VMEM((ITERS, COLS + 2, BOX + 16, LANES), jnp.float32),
        pltpu.VMEM((COLS, BOX, LANES), jnp.float32),
        pltpu.SemaphoreType.DMA,
        pltpu.SemaphoreType.DMA,
        pltpu.SemaphoreType.DMA,
    ]
    if begun:
        operands += [before[1], before[0]]
        in_specs += [SMEM, HBM]
        out_shape = [jax.ShapeDtypeStruct((2 * QUARTER, BOX, LANES), jnp.float32)] * 4
        out_specs = [HBM] * 4
        scratch = [pltpu.VMEM(whole, jnp.float32), pltpu.SemaphoreType.DMA((8,))] + scratch
    else:
        out_shape = [jax.ShapeDtypeStruct(whole, jnp.float32), jax.ShapeDtypeStruct((1,), jnp.int32)]
        out_specs = [VMEM, SMEM]
    return pl.pallas_call(
        functools.partial(pairs_kernel, begun),
        out_shape=out_shape,
        in_specs=in_specs,
        out_specs=out_specs,
        scratch_shapes=scratch,
        compiler_params=pltpu.CompilerParams(vmem_limit_bytes=VMEM_LIMIT),
        cost_estimate=pl.CostEstimate(flops=100_000_000, bytes_accessed=8 << 20, transcendentals=0),
        name="pairs_far" if begun else "pairs_near",
    )(*operands)


def settle_kernel(offsets, *refs):
    parts, sums, pieces, tall = refs[:6], refs[6:8], refs[8:13], refs[13]
    group, _ = place()
    for k in range(2):
        kept, once, twice = parts[3 * k : 3 * k + 3]
        tall[:, pl.ds(0, SLAB), :] = jnp.zeros((QUARTER, SLAB, LANES), jnp.float32)
        tall[:, pl.ds(SLAB + BOX, SLAB), :] = jnp.zeros((QUARTER, SLAB, LANES), jnp.float32)
        for c in range(QUARTER):
            value = (kept[c] + once[c]) + twice[c]
            sums[k][c] = value
            tall[c, pl.ds(SLAB, BOX), :] = value
        depth = offsets[(2 * group + k) * 3] - group * SLAB
        for t in range(SLABS):
            for c in range(QUARTER):
                pieces[t][k, c] = tall[c, pl.ds(SLAB * (t + 1) - depth, SLAB), :]


def settle(offsets, parts):
    quarter = jax.ShapeDtypeStruct((QUARTER, BOX, LANES), jnp.float32)
    piece = jax.ShapeDtypeStruct((2, QUARTER, SLAB, LANES), jnp.float32)
    block = pl.BlockSpec((QUARTER, BOX, LANES), lambda i: (0, 0, 0))
    return pl.pallas_call(
        settle_kernel,
        grid=(1,),
        out_shape=[quarter] * 2 + [piece] * SLABS,
        in_specs=[SMEM] + [block] * 6,
        out_specs=[block] * 2 + [pl.BlockSpec(piece.shape, lambda i: (0, 0, 0, 0))] * SLABS,
        scratch_shapes=[pltpu.VMEM((QUARTER, BOX + 2 * SLAB, LANES), jnp.float32)],
        cost_estimate=pl.CostEstimate(flops=4_000_000, bytes_accessed=4 << 20, transcendentals=0),
        name="settle",
    )(offsets, *parts)


def deposit_kernel(offsets, *refs):
    pieces, outs, span = refs[:SLABS], refs[SLABS : SLABS + 2], refs[-1]
    group, _ = place()
    lanes = lax.broadcasted_iota(jnp.int32, (SLAB, LANES), 1)
    span[...] = jnp.zeros_like(span)
    for t in range(SLABS):
        owner = (group + lax.axis_size("orb") - t) % lax.axis_size("orb")

        def lay(k, carry):
            at = (2 * owner + k) * 3
            base = offsets[at + 1] * WIDE + offsets[at + 2]
            for c in range(QUARTER):
                value = pieces[t][k, c]
                for row in range(2):
                    start = base + (2 * c + row) * WIDE - row * BOX
                    tile, turn = start >> 7, start & (LANES - 1)
                    kept = (lanes < BOX) if row == 0 else (lanes >= BOX)
                    turned = pltpu.roll(jnp.where(kept, value, 0.0), turn, 1)
                    here = pl.ds(pl.multiple_of(tile * LANES, LANES), LANES)
                    there = pl.ds(pl.multiple_of(tile * LANES + LANES, LANES), LANES)
                    span[:, here] = span[:, here] + jnp.where(lanes >= turn, turned, 0.0)
                    span[:, there] = span[:, there] + jnp.where(lanes < turn, turned, 0.0)
            return carry

        lax.fori_loop(0, 2, lay, 0)
    for half in range(2):
        outs[half][...] = span[pl.ds(8 * half, 8), pl.ds(0, SPAN)]


def deposit(offsets, pieces):
    half = jax.ShapeDtypeStruct((SLAB // 2, SPAN), jnp.float32)
    return pl.pallas_call(
        deposit_kernel,
        out_shape=[half] * 2,
        in_specs=[SMEM] + [VMEM] * SLABS,
        out_specs=[VMEM] * 2,
        scratch_shapes=[pltpu.VMEM((SLAB, SPAN + 4 * LANES), jnp.float32)],
        cost_estimate=pl.CostEstimate(flops=8_000_000, bytes_accessed=2 << 20, transcendentals=0),
        name="deposit",
    )(offsets, *pieces)


def quarters_of(mine):
    return mine, mine ^ 1, mine ^ 3, mine ^ 2


def merge_kernel(*refs):
    spans, out = refs[:8], refs[8]
    _, mine = place()
    out[...] = jnp.zeros_like(out)
    for n, quarter in enumerate(quarters_of(mine)):
        where = pl.ds(pl.multiple_of(quarter * (WIDE * BOX // 4), LANES), SPAN)
        for half in range(2):
            rows = pl.ds(8 * half, 8)
            out[rows, where] = out[rows, where] + spans[2 * n + half][...]


def merge(spans):
    return pl.pallas_call(
        merge_kernel,
        out_shape=jax.ShapeDtypeStruct((SLAB, WIDE * WIDE), jnp.float32),
        in_specs=[VMEM] * 8,
        out_specs=VMEM,
        cost_estimate=pl.CostEstimate(flops=1_000_000, bytes_accessed=2 << 20, transcendentals=0),
        name="merge",
    )(*spans)


def assemble_kernel(*refs):
    parts, out = refs[:8], refs[8]
    _, mine = place()
    for n, quarter in enumerate(quarters_of(mine)):
        for k in range(2):
            for c in range(QUARTER):
                where = pl.ds(pl.multiple_of((quarter * QUARTER + c) * LANES, LANES), LANES)
                out[k, :, where] = parts[2 * n + k][c]


def assemble(parts):
    return pl.pallas_call(
        assemble_kernel,
        out_shape=jax.ShapeDtypeStruct((2, BOX, BOX * BOX), jnp.float32),
        in_specs=[VMEM] * 8,
        out_specs=VMEM,
        cost_estimate=pl.CostEstimate(flops=1_000_000, bytes_accessed=4 << 20, transcendentals=0),
        name="assemble",
    )(*parts)


def across(block, side):
    return lax.ppermute(block, "rep", [(i, i ^ side) for i in range(lax.axis_size("rep"))])


def gather_pair(first, second):
    first_one, first_three = across(first, 1), across(first, 3)
    second_one, second_three = across(second, 1), across(second, 3)
    first_two = across(first_three, 1)
    second_two = across(second_one, 3)
    return [first, second, first_one, second_one, first_three, second_three, first_two, second_two]


def shards(orbitals, pair_list, box_offsets):
    groups = lax.axis_size("orb")
    to_near = [(g, g ^ 1) for g in range(groups)]
    to_far = [(g, neighbours(g)[1]) for g in range(groups) if 0 <= neighbours(g)[1] < groups]
    slots = pair_list.reshape(-1)
    known = jnp.concatenate([slots, lax.ppermute(slots, "orb", to_near), lax.ppermute(slots, "orb", to_far)])
    near = lax.ppermute(orbitals, "orb", to_near)
    far = lax.ppermute(orbitals, "orb", to_far)
    lists = jnp.concatenate([known] + [across(known, side) for side in (1, 2, 3)])
    offsets = box_offsets.reshape(-1)
    before = run_pairs(lists, offsets, orbitals, near)
    sent_zero, kept_zero, sent_one, kept_one = run_pairs(lists, offsets, orbitals, far, before)
    got_zero, got_one = across(sent_zero, 1), across(sent_one, 3)
    last_zero = across(kept_zero[QUARTER:] + got_zero[QUARTER:], 3)
    last_one = across(kept_one[QUARTER:] + got_one[QUARTER:], 1)
    settled = settle(offsets, (kept_zero, got_zero, last_zero, kept_one, got_one, last_one))
    pieces = [settled[2]]
    for later in range(1, SLABS):
        pieces.append(lax.ppermute(settled[2 + later], "orb", [(i, (i + later) % groups) for i in range(groups)]))
    forces = assemble(gather_pair(settled[0], settled[1]))
    slab = merge(gather_pair(*deposit(offsets, pieces)))
    return (forces, slab)


def solution(mesh):
    in_specs = (P("orb", None, None), P(("orb", "rep"), None), P())
    out_specs = (P("orb", None, None), P("orb", None))
    return jax.shard_map(shards, mesh=mesh, in_specs=in_specs, out_specs=out_specs, check_vma=False)
```

```python
import functools

import jax
import jax.numpy as jnp
import numpy as np
from jax import lax
from jax.experimental import pallas as pl
from jax.experimental.pallas import tpu as pltpu
from jax.sharding import PartitionSpec as P


BOX = 64
SLAB = 16
WIDE = 96
ITERS = 5
SCREEN = 6.1
LANES = 128
COLS = BOX * BOX // LANES
FRONT = 16
GROUP = 16
ROOM = 32
QUARTER = COLS // 4
SLABS = BOX // SLAB + 1
SPAN = WIDE * BOX // 4 + 32 * WIDE
PAIRS_VMEM = 32 * 1024 * 1024
SMALL_VMEM = 12 * 1024 * 1024
SMEM = pl.BlockSpec(memory_space=pltpu.SMEM)
VMEM = pl.BlockSpec(memory_space=pltpu.VMEM)
HBM = pl.BlockSpec(memory_space=pltpu.HBM)


def place():
    return lax.axis_index("orb"), lax.axis_index("rep")


def neighbours(group):
    return group ^ 1, group + 2 * (group & 1) - 1


def lane_of(rows):
    return lax.broadcasted_iota(jnp.int32, (rows, LANES), 1)


def fold(block):
    return jnp.sum(block.reshape(BOX // 8, 8, LANES), axis=0)


def total(partial):
    return jnp.sum(jnp.sum(partial, axis=1, keepdims=True), axis=0, keepdims=True)


def shift_reader(buffer, dz, dx, dy):
    lanes = lane_of(BOX)
    flat = dx * BOX + dy
    blocks = flat >> 7
    turn = flat & (LANES - 1)
    ypos = lanes & (BOX - 1)
    inside = (ypos >= dy) & (ypos < BOX + dy)
    early = lanes < LANES - turn

    def read(c):
        near = buffer[c - blocks + FRONT, pl.ds(ROOM - dz, BOX), :]
        before = buffer[c - blocks + FRONT - 1, pl.ds(ROOM - dz, BOX), :]
        turned = pltpu.roll(jnp.where(early, near, before), turn, 1)
        return jnp.where(inside, turned, 0.0)

    return read


def beside(field, c, center, after, within):
    above = field[c + 1, pl.ds(9, BOX), :]
    below = field[c + 1, pl.ds(7, BOX), :]
    ahead = field[c, pl.ds(8, BOX), :]
    across = pltpu.roll(jnp.where(lane_of(BOX) < BOX, after, ahead), BOX, 1)
    high = center.astype(jnp.bfloat16)
    low = (center - high.astype(jnp.float32)).astype(jnp.bfloat16)
    inner = jnp.dot(jnp.concatenate([high, low], axis=1), within[...], preferred_element_type=jnp.float32)
    return (inner + across) + (above + below)


def columns(c):
    return pl.ds(pl.multiple_of(c * LANES, LANES), LANES)


def load_box(own, other, which, write):
    for boxes, first in ((own, 0), (other, 2)):

        @pl.when((which >= first) & (which < first + 2))
        def _():
            def block(c, carry):
                write(c, boxes[which - first, :, columns(c)])
                return carry

            lax.fori_loop(0, COLS, block, 0, unroll=8)


def solve_pair(own, other, first, second, delta, within, buffer, still, shifted, basis, image):
    def to_buffer(c, block):
        buffer[c + FRONT, pl.ds(ROOM, BOX), :] = block

    def to_still(c, block):
        still[c] = block

    load_box(own, other, first, to_buffer)
    load_box(own, other, second, to_still)
    read = shift_reader(buffer, *delta)
    diagonal, coupling = [], []
    norm_before = None
    for k in range(ITERS):
        field = basis.at[k]

        def value_of(c):
            if k == 0:
                moved = read(c)
                shifted[c] = moved
                return still[c] * moved
            fresh = image[c] - diagonal[k - 1] * basis[k - 1, c + 1, pl.ds(8, BOX), :]
            if k > 1:
                fresh = fresh - coupling[k - 1] * basis[k - 2, c + 1, pl.ds(8, BOX), :]
            return fresh

        def group(start, carry, final):
            norm, cross = carry
            center = field[start + 1, pl.ds(8, BOX), :]
            values = [center]
            for u in range(1, GROUP + 1):
                if final and u == GROUP:
                    values.append(jnp.zeros_like(center))
                    continue
                fresh = value_of(start + u)
                field[start + u + 1, pl.ds(8, BOX), :] = fresh
                norm = norm + fold(fresh * fresh)
                values.append(fresh)
            for u in range(GROUP):
                result = beside(field, start + u, values[u], values[u + 1], within)
                if k < ITERS - 1:
                    image[start + u] = result
                cross = cross + fold(values[u] * result)
            return norm, cross

        opening = value_of(0)
        field[1, pl.ds(8, BOX), :] = opening
        carry = (fold(opening * opening), jnp.zeros((8, LANES), jnp.float32))
        carry = lax.fori_loop(0, COLS // GROUP - 1, lambda m, held: group(m * GROUP, held, False), carry)
        norm, cross = group(COLS - GROUP, carry, True)
        norm = total(norm)
        diagonal.append(total(cross) / norm)
        coupling.append(norm / norm_before if k > 0 else None)
        norm_before = norm
    pivots = [SCREEN - diagonal[0]]
    rights = [jnp.ones_like(pivots[0])]
    for k in range(1, ITERS):
        pivots.append(SCREEN - diagonal[k] - coupling[k] / pivots[k - 1])
        rights.append(rights[k - 1] / pivots[k - 1])
    weights = [None] * ITERS
    weights[ITERS - 1] = rights[ITERS - 1] / pivots[ITERS - 1]
    for k in range(ITERS - 2, -1, -1):
        weights[k] = (rights[k] + coupling[k + 1] * weights[k + 1]) / pivots[k]
    return weights


def run_pair(own, other, first, second, delta, to_second, to_first, within, forces, *scratch):
    buffer, still, shifted, basis, image = scratch
    weights = solve_pair(own, other, first, second, delta, within, *scratch)

    def finish(c, carry):
        potential = weights[0] * basis[0, c + 1, pl.ds(8, BOX), :]
        for k in range(1, ITERS):
            potential = potential + weights[k] * basis[k, c + 1, pl.ds(8, BOX), :]
        image[c] = potential
        buffer[c + FRONT, pl.ds(ROOM, BOX), :] = potential * still[c]
        return carry

    lax.fori_loop(0, COLS, finish, 0, unroll=4)

    @pl.when(to_second)
    def _():
        def deposit(c, carry):
            forces[second, c] = forces[second, c] + image[c] * shifted[c]
            return carry

        lax.fori_loop(0, COLS, deposit, 0, unroll=4)

    @pl.when(to_first)
    def _():
        read = shift_reader(buffer, -delta[0], -delta[1], -delta[2])

        def deposit(c, carry):
            forces[first, c] = forces[first, c] + read(c)
            return carry

        lax.fori_loop(0, COLS, deposit, 0, unroll=8)


def pairs_kernel(begun, *refs):
    if begun:
        lists, offsets, own, other, within, tally, forces_in, *parts, forces = refs[:12]
    else:
        lists, offsets, own, other, within, forces, tally_out = refs[:7]
    scratch = refs[-5:]
    buffer, basis = scratch[0], scratch[3]
    group, mine = place()
    near, far = neighbours(group)
    neighbour, which = (far, 2) if begun else (near, 1)

    def clear(c, carry):
        buffer[c] = jnp.zeros((BOX + 2 * ROOM, LANES), jnp.float32)
        return carry

    lax.fori_loop(0, COLS + 2 * FRONT, clear, 0, unroll=4)
    nothing = jnp.zeros((BOX + 16, LANES), jnp.float32)
    for k in range(ITERS):
        basis[k, 0] = nothing
        basis[k, COLS + 1] = nothing

        def clear_ends(c, carry):
            basis[k, c + 1, pl.ds(0, 8), :] = jnp.zeros((8, LANES), jnp.float32)
            basis[k, c + 1, pl.ds(BOX + 8, 8), :] = jnp.zeros((8, LANES), jnp.float32)
            return carry

        lax.fori_loop(0, COLS, clear_ends, 0, unroll=4)

    def open_forces(c, carry):
        for k in range(2):
            forces[k, c] = forces_in[k, c] if begun else jnp.zeros((BOX, LANES), jnp.float32)
        return carry

    lax.fori_loop(0, COLS, open_forces, 0, unroll=2)

    def slot(n, count):
        foreign = n // 16
        row = n % 16
        base = ((row // 4) ^ mine) * 36 + foreign * which * 12 + (row % 4) * 3
        first = lists[base]
        second = lists[base + 1]
        live = lists[base + 2] > 0
        second_group = second // 2
        inner = second_group == group
        outer = second_group == neighbour
        if begun:
            wanted = jnp.where(foreign > 0, inner, outer)
        else:
            wanted = jnp.where(foreign > 0, inner, inner | outer)
        taken = live & wanted
        turn = taken & (lax.rem(count, 4) == mine)

        @pl.when(turn)
        def _():
            delta = [offsets[first * 3 + axis] - offsets[second * 3 + axis] for axis in range(3)]
            first_at = jnp.where(foreign > 0, 2 + first - 2 * neighbour, first - 2 * group)
            second_at = jnp.where(inner, second - 2 * group, 2 + second - 2 * neighbour)
            run_pair(own, other, first_at, second_at, delta, inner, foreign == 0, within, forces, *scratch)

        return count + taken.astype(jnp.int32)

    if not begun:
        tally_out[0] = lax.fori_loop(0, 32, slot, jnp.int32(0))
        return
    lax.fori_loop(0, 32, slot, tally[0])
    for k, side in enumerate((1, 3)):
        for n, who in enumerate((mine ^ side, mine)):
            for half, quarter in enumerate((who, who ^ (4 - side))):
                for c in range(QUARTER):
                    parts[2 * k + n][half * QUARTER + c] = forces[k, quarter * QUARTER + c]


def within_block():
    lane = np.arange(LANES)
    gap = np.abs(lane[:, None] - lane[None, :])
    same_row = lane[:, None] // BOX == lane[None, :] // BOX
    once = ((gap == 1) & same_row) | (gap == BOX)
    return jnp.asarray(np.concatenate([once, once]), jnp.bfloat16)


def stage_kernel(boxes, out):
    pltpu.sync_copy(boxes, out)


def stage(boxes):
    return pl.pallas_call(
        stage_kernel,
        out_shape=jax.ShapeDtypeStruct(boxes.shape, boxes.dtype),
        in_specs=[HBM],
        out_specs=VMEM,
        compiler_params=pltpu.CompilerParams(vmem_limit_bytes=SMALL_VMEM),
        cost_estimate=pl.CostEstimate(flops=1_000_000, bytes_accessed=4 << 20, transcendentals=0),
        name="stage",
    )(boxes)


def run_pairs(lists, offsets, own, other, before=None):
    begun = before is not None
    operands = [lists, offsets, own, other, within_block()]
    in_specs = [SMEM, SMEM, VMEM, VMEM, VMEM]
    whole = (2, COLS, BOX, LANES)
    scratch = [
        pltpu.VMEM((COLS + 2 * FRONT, BOX + 2 * ROOM, LANES), jnp.float32),
        pltpu.VMEM((COLS, BOX, LANES), jnp.float32),
        pltpu.VMEM((COLS, BOX, LANES), jnp.float32),
        pltpu.VMEM((ITERS, COLS + 2, BOX + 16, LANES), jnp.float32),
        pltpu.VMEM((COLS, BOX, LANES), jnp.float32),
    ]
    if begun:
        operands += [before[1], before[0]]
        in_specs += [SMEM, VMEM]
        out_shape = [jax.ShapeDtypeStruct((2 * QUARTER, BOX, LANES), jnp.float32)] * 4
        out_specs = [VMEM] * 4
        scratch = [pltpu.VMEM(whole, jnp.float32)] + scratch
    else:
        out_shape = [jax.ShapeDtypeStruct(whole, jnp.float32), jax.ShapeDtypeStruct((1,), jnp.int32)]
        out_specs = [VMEM, SMEM]
    return pl.pallas_call(
        functools.partial(pairs_kernel, begun),
        out_shape=out_shape,
        in_specs=in_specs,
        out_specs=out_specs,
        scratch_shapes=scratch,
        compiler_params=pltpu.CompilerParams(vmem_limit_bytes=PAIRS_VMEM),
        cost_estimate=pl.CostEstimate(flops=100_000_000, bytes_accessed=8 << 20, transcendentals=0),
        name="pairs_far" if begun else "pairs_near",
    )(*operands)


def settle_kernel(offsets, *refs):
    parts, sums, pieces, tall = refs[:6], refs[6:8], refs[8:13], refs[13]
    group, _ = place()
    for k in range(2):
        kept, once, twice = parts[3 * k : 3 * k + 3]
        tall[:, pl.ds(0, SLAB), :] = jnp.zeros((QUARTER, SLAB, LANES), jnp.float32)
        tall[:, pl.ds(SLAB + BOX, SLAB), :] = jnp.zeros((QUARTER, SLAB, LANES), jnp.float32)
        for c in range(QUARTER):
            value = (kept[c] + once[c]) + twice[c]
            sums[k][c] = value
            tall[c, pl.ds(SLAB, BOX), :] = value
        depth = offsets[(2 * group + k) * 3] - group * SLAB
        for t in range(SLABS):
            for c in range(QUARTER):
                pieces[t][k, c] = tall[c, pl.ds(SLAB * (t + 1) - depth, SLAB), :]


def settle(offsets, parts):
    quarter = jax.ShapeDtypeStruct((QUARTER, BOX, LANES), jnp.float32)
    piece = jax.ShapeDtypeStruct((2, QUARTER, SLAB, LANES), jnp.float32)
    return pl.pallas_call(
        settle_kernel,
        out_shape=[quarter] * 2 + [piece] * SLABS,
        in_specs=[SMEM] + [VMEM] * 6,
        out_specs=[VMEM] * (2 + SLABS),
        scratch_shapes=[pltpu.VMEM((QUARTER, BOX + 2 * SLAB, LANES), jnp.float32)],
        cost_estimate=pl.CostEstimate(flops=4_000_000, bytes_accessed=4 << 20, transcendentals=0),
        compiler_params=pltpu.CompilerParams(vmem_limit_bytes=SMALL_VMEM),
        name="settle",
    )(offsets, *parts)


def deposit_kernel(offsets, *refs):
    pieces, outs, span = refs[:SLABS], refs[SLABS : SLABS + 2], refs[-1]
    group, _ = place()
    lanes = lax.broadcasted_iota(jnp.int32, (SLAB, LANES), 1)
    span[...] = jnp.zeros_like(span)
    for t in range(SLABS):
        owner = (group + lax.axis_size("orb") - t) % lax.axis_size("orb")

        def lay(k, carry):
            at = (2 * owner + k) * 3
            base = offsets[at + 1] * WIDE + offsets[at + 2]
            for c in range(QUARTER):
                value = pieces[t][k, c]
                for row in range(2):
                    start = base + (2 * c + row) * WIDE - row * BOX
                    tile, turn = start >> 7, start & (LANES - 1)
                    kept = (lanes < BOX) if row == 0 else (lanes >= BOX)
                    turned = pltpu.roll(jnp.where(kept, value, 0.0), turn, 1)
                    here = pl.ds(pl.multiple_of(tile * LANES, LANES), LANES)
                    there = pl.ds(pl.multiple_of(tile * LANES + LANES, LANES), LANES)
                    span[:, here] = span[:, here] + jnp.where(lanes >= turn, turned, 0.0)
                    span[:, there] = span[:, there] + jnp.where(lanes < turn, turned, 0.0)
            return carry

        lax.fori_loop(0, 2, lay, 0)
    for half in range(2):
        outs[half][...] = span[pl.ds(8 * half, 8), pl.ds(0, SPAN)]


def deposit(offsets, pieces):
    half = jax.ShapeDtypeStruct((SLAB // 2, SPAN), jnp.float32)
    return pl.pallas_call(
        deposit_kernel,
        out_shape=[half] * 2,
        in_specs=[SMEM] + [VMEM] * SLABS,
        out_specs=[VMEM] * 2,
        scratch_shapes=[pltpu.VMEM((SLAB, SPAN + 4 * LANES), jnp.float32)],
        cost_estimate=pl.CostEstimate(flops=8_000_000, bytes_accessed=2 << 20, transcendentals=0),
        compiler_params=pltpu.CompilerParams(vmem_limit_bytes=SMALL_VMEM),
        name="deposit",
    )(offsets, *pieces)


def quarters_of(mine):
    return mine, mine ^ 1, mine ^ 3, mine ^ 2


def merge_kernel(*refs):
    spans, out = refs[:8], refs[8]
    _, mine = place()
    out[...] = jnp.zeros_like(out)
    for n, quarter in enumerate(quarters_of(mine)):
        where = pl.ds(pl.multiple_of(quarter * (WIDE * BOX // 4), LANES), SPAN)
        for half in range(2):
            rows = pl.ds(8 * half, 8)
            out[rows, where] = out[rows, where] + spans[2 * n + half][...]


def merge(spans):
    return pl.pallas_call(
        merge_kernel,
        out_shape=jax.ShapeDtypeStruct((SLAB, WIDE * WIDE), jnp.float32),
        in_specs=[VMEM] * 8,
        out_specs=VMEM,
        cost_estimate=pl.CostEstimate(flops=1_000_000, bytes_accessed=2 << 20, transcendentals=0),
        compiler_params=pltpu.CompilerParams(vmem_limit_bytes=SMALL_VMEM),
        name="merge",
    )(*spans)


def assemble_kernel(*refs):
    parts, out = refs[:8], refs[8]
    _, mine = place()
    for n, quarter in enumerate(quarters_of(mine)):
        for k in range(2):
            for c in range(QUARTER):
                where = pl.ds(pl.multiple_of((quarter * QUARTER + c) * LANES, LANES), LANES)
                out[k, :, where] = parts[2 * n + k][c]


def assemble(parts):
    return pl.pallas_call(
        assemble_kernel,
        out_shape=jax.ShapeDtypeStruct((2, BOX, BOX * BOX), jnp.float32),
        in_specs=[VMEM] * 8,
        out_specs=VMEM,
        cost_estimate=pl.CostEstimate(flops=1_000_000, bytes_accessed=4 << 20, transcendentals=0),
        compiler_params=pltpu.CompilerParams(vmem_limit_bytes=SMALL_VMEM),
        name="assemble",
    )(*parts)


def across(block, side):
    return lax.ppermute(block, "rep", [(i, i ^ side) for i in range(lax.axis_size("rep"))])


def gather_pair(first, second):
    first_one, first_three = across(first, 1), across(first, 3)
    second_one, second_three = across(second, 1), across(second, 3)
    first_two = across(first_three, 1)
    second_two = across(second_one, 3)
    return [first, second, first_one, second_one, first_three, second_three, first_two, second_two]


def shards(orbitals, pair_list, box_offsets):
    groups = lax.axis_size("orb")
    to_near = [(g, g ^ 1) for g in range(groups)]
    to_far = [(g, neighbours(g)[1]) for g in range(groups) if 0 <= neighbours(g)[1] < groups]
    slots = pair_list.reshape(-1)
    near_slots = lax.ppermute(slots, "orb", to_near)
    far_slots = lax.ppermute(slots, "orb", to_far)
    near = lax.ppermute(orbitals, "orb", to_near)
    far = lax.ppermute(orbitals, "orb", to_far)
    known = jnp.concatenate([slots, near_slots, far_slots])
    lists = jnp.concatenate([known] + [across(known, side) for side in (1, 2, 3)])
    offsets = box_offsets.reshape(-1)
    own = stage(orbitals)
    before = run_pairs(lists, offsets, own, near)
    sent_zero, kept_zero, sent_one, kept_one = run_pairs(lists, offsets, own, far, before)
    got_zero, got_one = across(sent_zero, 1), across(sent_one, 3)
    last_zero = across(kept_zero[QUARTER:] + got_zero[QUARTER:], 3)
    last_one = across(kept_one[QUARTER:] + got_one[QUARTER:], 1)
    settled = settle(offsets, (kept_zero, got_zero, last_zero, kept_one, got_one, last_one))
    pieces = [settled[2]]
    for later in range(1, SLABS):
        route = [(i, (i + later) % groups) for i in range(groups)]
        pieces.append(lax.ppermute(settled[2 + later], "orb", route))
    gathered = gather_pair(settled[0], settled[1])
    forces = assemble(gathered)
    spans = deposit(offsets, pieces)
    gathered = gather_pair(*spans)
    slab = merge(gathered)
    return (forces, slab)


def solution(mesh):
    in_specs = (P("orb", None, None), P(("orb", "rep"), None), P())
    out_specs = (P("orb", None, None), P("orb", None))
    return jax.shard_map(shards, mesh=mesh, in_specs=in_specs, out_specs=out_specs, check_vma=False)
```

```python
import functools

import jax
import jax.numpy as jnp
import numpy as np
from jax import lax
from jax.experimental import pallas as pl
from jax.experimental.pallas import tpu as pltpu
from jax.sharding import PartitionSpec as P


BOX = 64
SLAB = 16
WIDE = 96
ITERS = 5
SCREEN = 6.1
LANES = 128
COLS = BOX * BOX // LANES
FRONT = 16
GROUP = 16
ROOM = 32
QUARTER = COLS // 4
SLABS = BOX // SLAB + 1
SPAN = WIDE * BOX // 4 + 32 * WIDE
PAIRS_VMEM = 32 * 1024 * 1024
SMALL_VMEM = 12 * 1024 * 1024
SMEM = pl.BlockSpec(memory_space=pltpu.SMEM)
VMEM = pl.BlockSpec(memory_space=pltpu.VMEM)
HBM = pl.BlockSpec(memory_space=pltpu.HBM)


def place():
    return lax.axis_index("orb"), lax.axis_index("rep")


def neighbours(group):
    return group ^ 1, group + 2 * (group & 1) - 1


def lane_of(rows):
    return lax.broadcasted_iota(jnp.int32, (rows, LANES), 1)


def fold(block):
    return jnp.sum(block.reshape(BOX // 8, 8, LANES), axis=0)


def total(partial):
    return jnp.sum(jnp.sum(partial, axis=1, keepdims=True), axis=0, keepdims=True)


def shift_reader(buffer, dz, dx, dy):
    lanes = lane_of(BOX)
    flat = dx * BOX + dy
    blocks = flat >> 7
    turn = flat & (LANES - 1)
    ypos = lanes & (BOX - 1)
    inside = (ypos >= dy) & (ypos < BOX + dy)
    early = lanes < LANES - turn

    def read(c):
        near = buffer[c - blocks + FRONT, pl.ds(ROOM - dz, BOX), :]
        before = buffer[c - blocks + FRONT - 1, pl.ds(ROOM - dz, BOX), :]
        turned = pltpu.roll(jnp.where(early, near, before), turn, 1)
        return jnp.where(inside, turned, 0.0)

    return read


def beside(field, c, center, after, within):
    above = field[c + 1, pl.ds(9, BOX), :]
    below = field[c + 1, pl.ds(7, BOX), :]
    ahead = field[c, pl.ds(8, BOX), :]
    across = pltpu.roll(jnp.where(lane_of(BOX) < BOX, after, ahead), BOX, 1)
    high = center.astype(jnp.bfloat16)
    low = (center - high.astype(jnp.float32)).astype(jnp.bfloat16)
    inner = jnp.dot(jnp.concatenate([high, low], axis=1), within[...], preferred_element_type=jnp.float32)
    return (inner + across) + (above + below)


def columns(c):
    return pl.ds(pl.multiple_of(c * LANES, LANES), LANES)


def load_box(own, other, which, write):
    for boxes, first in ((own, 0), (other, 2)):

        @pl.when((which >= first) & (which < first + 2))
        def _():
            def block(c, carry):
                write(c, boxes[which - first, :, columns(c)])
                return carry

            lax.fori_loop(0, COLS, block, 0, unroll=8)


def solve_pair(own, other, first, second, delta, within, buffer, still, shifted, basis, image):
    def to_buffer(c, block):
        buffer[c + FRONT, pl.ds(ROOM, BOX), :] = block

    def to_still(c, block):
        still[c] = block

    load_box(own, other, first, to_buffer)
    load_box(own, other, second, to_still)
    read = shift_reader(buffer, *delta)
    diagonal, coupling = [], []
    norm_before = None
    for k in range(ITERS):
        field = basis.at[k]

        def value_of(c):
            if k == 0:
                moved = read(c)
                shifted[c] = moved
                return still[c] * moved
            fresh = image[c] - diagonal[k - 1] * basis[k - 1, c + 1, pl.ds(8, BOX), :]
            if k > 1:
                fresh = fresh - coupling[k - 1] * basis[k - 2, c + 1, pl.ds(8, BOX), :]
            return fresh

        def group(start, carry, final):
            norm, cross = carry
            center = field[start + 1, pl.ds(8, BOX), :]
            values = [center]
            for u in range(1, GROUP + 1):
                if final and u == GROUP:
                    values.append(jnp.zeros_like(center))
                    continue
                fresh = value_of(start + u)
                field[start + u + 1, pl.ds(8, BOX), :] = fresh
                norm = norm + fold(fresh * fresh)
                values.append(fresh)
            for u in range(GROUP):
                result = beside(field, start + u, values[u], values[u + 1], within)
                if k < ITERS - 1:
                    image[start + u] = result
                cross = cross + fold(values[u] * result)
            return norm, cross

        opening = value_of(0)
        field[1, pl.ds(8, BOX), :] = opening
        carry = (fold(opening * opening), jnp.zeros((8, LANES), jnp.float32))
        carry = lax.fori_loop(0, COLS // GROUP - 1, lambda m, held: group(m * GROUP, held, False), carry)
        norm, cross = group(COLS - GROUP, carry, True)
        norm = total(norm)
        diagonal.append(total(cross) / norm)
        coupling.append(norm / norm_before if k > 0 else None)
        norm_before = norm
    pivots = [SCREEN - diagonal[0]]
    rights = [jnp.ones_like(pivots[0])]
    for k in range(1, ITERS):
        pivots.append(SCREEN - diagonal[k] - coupling[k] / pivots[k - 1])
        rights.append(rights[k - 1] / pivots[k - 1])
    weights = [None] * ITERS
    weights[ITERS - 1] = rights[ITERS - 1] / pivots[ITERS - 1]
    for k in range(ITERS - 2, -1, -1):
        weights[k] = (rights[k] + coupling[k + 1] * weights[k + 1]) / pivots[k]
    return weights


def run_pair(own, other, first, second, delta, to_second, to_first, within, forces, *scratch):
    buffer, still, shifted, basis, image = scratch
    weights = solve_pair(own, other, first, second, delta, within, *scratch)

    def finish(c, carry):
        potential = weights[0] * basis[0, c + 1, pl.ds(8, BOX), :]
        for k in range(1, ITERS):
            potential = potential + weights[k] * basis[k, c + 1, pl.ds(8, BOX), :]
        image[c] = potential
        buffer[c + FRONT, pl.ds(ROOM, BOX), :] = potential * still[c]
        return carry

    lax.fori_loop(0, COLS, finish, 0, unroll=4)

    @pl.when(to_second)
    def _():
        def deposit(c, carry):
            forces[second, c] = forces[second, c] + image[c] * shifted[c]
            return carry

        lax.fori_loop(0, COLS, deposit, 0, unroll=4)

    @pl.when(to_first)
    def _():
        read = shift_reader(buffer, -delta[0], -delta[1], -delta[2])

        def deposit(c, carry):
            forces[first, c] = forces[first, c] + read(c)
            return carry

        lax.fori_loop(0, COLS, deposit, 0, unroll=8)


def pairs_kernel(begun, *refs):
    if begun:
        lists, offsets, own, other_far, within, tally, forces_in, *parts, forces = refs[:12]
    else:
        lists, offsets, own, other_far, within, forces, tally_out = refs[:7]
    other, other_sem, *scratch = refs[-7:]
    buffer, basis = scratch[0], scratch[3]
    group, mine = place()
    near, far = neighbours(group)
    neighbour, which = (far, 2) if begun else (near, 1)
    copy = pltpu.make_async_copy(other_far, other, other_sem)
    copy.start()

    def clear(c, carry):
        buffer[c] = jnp.zeros((BOX + 2 * ROOM, LANES), jnp.float32)
        return carry

    lax.fori_loop(0, COLS + 2 * FRONT, clear, 0, unroll=4)
    nothing = jnp.zeros((BOX + 16, LANES), jnp.float32)
    for k in range(ITERS):
        basis[k, 0] = nothing

        def clear_ends(c, carry):
            basis[k, c + 1, pl.ds(0, 8), :] = jnp.zeros((8, LANES), jnp.float32)
            basis[k, c + 1, pl.ds(BOX + 8, 8), :] = jnp.zeros((8, LANES), jnp.float32)
            return carry

        lax.fori_loop(0, COLS, clear_ends, 0, unroll=4)

    def open_forces(c, carry):
        for k in range(2):
            forces[k, c] = forces_in[k, c] if begun else jnp.zeros((BOX, LANES), jnp.float32)
        return carry

    lax.fori_loop(0, COLS, open_forces, 0, unroll=2)
    copy.wait()

    def slot(n, count):
        foreign = n >> 4
        row = n & 15
        base = ((row >> 2) ^ mine) * 36 + foreign * (which * 12) + (row & 3) * 3
        first = lists[base]
        second = lists[base + 1]
        live = lists[base + 2] > 0
        second_group = second >> 1
        inner = second_group == group
        outer = second_group == neighbour
        if begun:
            wanted = jnp.where(foreign > 0, inner, outer)
        else:
            wanted = jnp.where(foreign > 0, inner, inner | outer)
        taken = live & wanted
        turn = taken & ((count & 3) == mine)

        @pl.when(turn)
        def _():
            delta = [offsets[first * 3 + axis] - offsets[second * 3 + axis] for axis in range(3)]
            first_at = jnp.where(foreign > 0, 2 + first - 2 * neighbour, first - 2 * group)
            second_at = jnp.where(inner, second - 2 * group, 2 + second - 2 * neighbour)
            run_pair(own, other, first_at, second_at, delta, inner, foreign == 0, within, forces, *scratch)

        return count + taken.astype(jnp.int32)

    if not begun:
        tally_out[0] = lax.fori_loop(0, 32, slot, jnp.int32(0))
        return
    lax.fori_loop(0, 32, slot, tally[0])
    for k, side in enumerate((1, 3)):
        for n, who in enumerate((mine ^ side, mine)):
            for half, quarter in enumerate((who, who ^ (4 - side))):
                for c in range(QUARTER):
                    parts[2 * k + n][half * QUARTER + c] = forces[k, quarter * QUARTER + c]


def within_block():
    lane = np.arange(LANES)
    gap = np.abs(lane[:, None] - lane[None, :])
    same_row = lane[:, None] // BOX == lane[None, :] // BOX
    once = ((gap == 1) & same_row) | (gap == BOX)
    return jnp.asarray(np.concatenate([once, once]), jnp.bfloat16)


def stage_kernel(boxes, out):
    pltpu.sync_copy(boxes, out)


def stage(boxes):
    return pl.pallas_call(
        stage_kernel,
        out_shape=jax.ShapeDtypeStruct(boxes.shape, boxes.dtype),
        in_specs=[HBM],
        out_specs=VMEM,
        compiler_params=pltpu.CompilerParams(vmem_limit_bytes=SMALL_VMEM),
        cost_estimate=pl.CostEstimate(flops=1_000_000, bytes_accessed=4 << 20, transcendentals=0),
        name="stage",
    )(boxes)


def run_pairs(lists, offsets, own, other, before=None):
    begun = before is not None
    operands = [lists, offsets, own, other, within_block()]
    in_specs = [SMEM, SMEM, VMEM, HBM, VMEM]
    whole = (2, COLS, BOX, LANES)
    scratch = [
        pltpu.VMEM((2, BOX, BOX * BOX), jnp.float32),
        pltpu.SemaphoreType.DMA,
        pltpu.VMEM((COLS + 2 * FRONT, BOX + 2 * ROOM, LANES), jnp.float32),
        pltpu.VMEM((COLS, BOX, LANES), jnp.float32),
        pltpu.VMEM((COLS, BOX, LANES), jnp.float32),
        pltpu.VMEM((ITERS, COLS + 1, BOX + 16, LANES), jnp.float32),
        pltpu.VMEM((COLS, BOX, LANES), jnp.float32),
    ]
    if begun:
        operands += [before[1], before[0]]
        in_specs += [SMEM, VMEM]
        out_shape = [jax.ShapeDtypeStruct((2 * QUARTER, BOX, LANES), jnp.float32)] * 4
        out_specs = [VMEM] * 4
        scratch = [pltpu.VMEM(whole, jnp.float32)] + scratch
    else:
        out_shape = [jax.ShapeDtypeStruct(whole, jnp.float32), jax.ShapeDtypeStruct((1,), jnp.int32)]
        out_specs = [VMEM, SMEM]
    return pl.pallas_call(
        functools.partial(pairs_kernel, begun),
        out_shape=out_shape,
        in_specs=in_specs,
        out_specs=out_specs,
        scratch_shapes=scratch,
        compiler_params=pltpu.CompilerParams(vmem_limit_bytes=PAIRS_VMEM),
        cost_estimate=pl.CostEstimate(flops=100_000_000, bytes_accessed=8 << 20, transcendentals=0),
        name="pairs_far" if begun else "pairs_near",
    )(*operands)


def settle_kernel(offsets, *refs):
    parts, sums, pieces, tall = refs[:6], refs[6:8], refs[8:13], refs[13]
    group, _ = place()
    for k in range(2):
        kept, once, twice = parts[3 * k : 3 * k + 3]
        tall[:, pl.ds(0, SLAB), :] = jnp.zeros((QUARTER, SLAB, LANES), jnp.float32)
        tall[:, pl.ds(SLAB + BOX, SLAB), :] = jnp.zeros((QUARTER, SLAB, LANES), jnp.float32)
        for c in range(QUARTER):
            value = (kept[c] + once[c]) + twice[c]
            sums[k][c] = value
            tall[c, pl.ds(SLAB, BOX), :] = value
        depth = offsets[(2 * group + k) * 3] - group * SLAB
        for t in range(SLABS):
            for c in range(QUARTER):
                pieces[t][k, c] = tall[c, pl.ds(SLAB * (t + 1) - depth, SLAB), :]


def settle(offsets, parts):
    quarter = jax.ShapeDtypeStruct((QUARTER, BOX, LANES), jnp.float32)
    piece = jax.ShapeDtypeStruct((2, QUARTER, SLAB, LANES), jnp.float32)
    return pl.pallas_call(
        settle_kernel,
        out_shape=[quarter] * 2 + [piece] * SLABS,
        in_specs=[SMEM] + [VMEM] * 6,
        out_specs=[VMEM] * (2 + SLABS),
        scratch_shapes=[pltpu.VMEM((QUARTER, BOX + 2 * SLAB, LANES), jnp.float32)],
        cost_estimate=pl.CostEstimate(flops=4_000_000, bytes_accessed=4 << 20, transcendentals=0),
        compiler_params=pltpu.CompilerParams(vmem_limit_bytes=SMALL_VMEM),
        name="settle",
    )(offsets, *parts)


def deposit_kernel(offsets, *refs):
    pieces, outs, span = refs[:SLABS], refs[SLABS : SLABS + 2], refs[-1]
    group, _ = place()
    lanes = lax.broadcasted_iota(jnp.int32, (SLAB, LANES), 1)
    span[...] = jnp.zeros_like(span)
    for t in range(SLABS):
        owner = (group + lax.axis_size("orb") - t) % lax.axis_size("orb")

        def lay(k, carry):
            at = (2 * owner + k) * 3
            base = offsets[at + 1] * WIDE + offsets[at + 2]
            for c in range(QUARTER):
                value = pieces[t][k, c]
                for row in range(2):
                    start = base + (2 * c + row) * WIDE - row * BOX
                    tile, turn = start >> 7, start & (LANES - 1)
                    kept = (lanes < BOX) if row == 0 else (lanes >= BOX)
                    turned = pltpu.roll(jnp.where(kept, value, 0.0), turn, 1)
                    here = pl.ds(pl.multiple_of(tile * LANES, LANES), LANES)
                    there = pl.ds(pl.multiple_of(tile * LANES + LANES, LANES), LANES)
                    span[:, here] = span[:, here] + jnp.where(lanes >= turn, turned, 0.0)
                    span[:, there] = span[:, there] + jnp.where(lanes < turn, turned, 0.0)
            return carry

        lax.fori_loop(0, 2, lay, 0)
    for half in range(2):
        outs[half][...] = span[pl.ds(8 * half, 8), pl.ds(0, SPAN)]


def deposit(offsets, pieces):
    half = jax.ShapeDtypeStruct((SLAB // 2, SPAN), jnp.float32)
    return pl.pallas_call(
        deposit_kernel,
        out_shape=[half] * 2,
        in_specs=[SMEM] + [VMEM] * SLABS,
        out_specs=[VMEM] * 2,
        scratch_shapes=[pltpu.VMEM((SLAB, SPAN + 4 * LANES), jnp.float32)],
        cost_estimate=pl.CostEstimate(flops=8_000_000, bytes_accessed=2 << 20, transcendentals=0),
        compiler_params=pltpu.CompilerParams(vmem_limit_bytes=SMALL_VMEM),
        name="deposit",
    )(offsets, *pieces)


def quarters_of(mine):
    return mine, mine ^ 1, mine ^ 3, mine ^ 2


def merge_kernel(*refs):
    spans, out = refs[:8], refs[8]
    _, mine = place()
    out[...] = jnp.zeros_like(out)
    for n, quarter in enumerate(quarters_of(mine)):
        where = pl.ds(pl.multiple_of(quarter * (WIDE * BOX // 4), LANES), SPAN)
        for half in range(2):
            rows = pl.ds(8 * half, 8)
            out[rows, where] = out[rows, where] + spans[2 * n + half][...]


def merge(spans):
    return pl.pallas_call(
        merge_kernel,
        out_shape=jax.ShapeDtypeStruct((SLAB, WIDE * WIDE), jnp.float32),
        in_specs=[VMEM] * 8,
        out_specs=VMEM,
        cost_estimate=pl.CostEstimate(flops=1_000_000, bytes_accessed=2 << 20, transcendentals=0),
        compiler_params=pltpu.CompilerParams(vmem_limit_bytes=SMALL_VMEM),
        name="merge",
    )(*spans)


def assemble_kernel(*refs):
    parts, out = refs[:8], refs[8]
    _, mine = place()
    for n, quarter in enumerate(quarters_of(mine)):
        for k in range(2):
            for c in range(QUARTER):
                where = pl.ds(pl.multiple_of((quarter * QUARTER + c) * LANES, LANES), LANES)
                out[k, :, where] = parts[2 * n + k][c]


def assemble(parts):
    return pl.pallas_call(
        assemble_kernel,
        out_shape=jax.ShapeDtypeStruct((2, BOX, BOX * BOX), jnp.float32),
        in_specs=[VMEM] * 8,
        out_specs=VMEM,
        cost_estimate=pl.CostEstimate(flops=1_000_000, bytes_accessed=4 << 20, transcendentals=0),
        compiler_params=pltpu.CompilerParams(vmem_limit_bytes=SMALL_VMEM),
        name="assemble",
    )(*parts)


def across(block, side):
    return lax.ppermute(block, "rep", [(i, i ^ side) for i in range(lax.axis_size("rep"))])


def gather_pair(first, second):
    first_one, first_three = across(first, 1), across(first, 3)
    second_one, second_three = across(second, 1), across(second, 3)
    first_two = across(first_three, 1)
    second_two = across(second_one, 3)
    return [first, second, first_one, second_one, first_three, second_three, first_two, second_two]


def shards(orbitals, pair_list, box_offsets):
    groups = lax.axis_size("orb")
    to_near = [(g, g ^ 1) for g in range(groups)]
    to_far = [(g, neighbours(g)[1]) for g in range(groups) if 0 <= neighbours(g)[1] < groups]
    slots = pair_list.reshape(-1)
    near_slots = lax.ppermute(slots, "orb", to_near)
    far_slots = lax.ppermute(slots, "orb", to_far)
    near = lax.ppermute(orbitals, "orb", to_near)
    far = lax.ppermute(orbitals, "orb", to_far)
    known = jnp.concatenate([slots, near_slots, far_slots])
    lists = jnp.concatenate([known] + [across(known, side) for side in (1, 2, 3)])
    offsets = box_offsets.reshape(-1)
    own = stage(orbitals)
    before = run_pairs(lists, offsets, own, near)
    sent_zero, kept_zero, sent_one, kept_one = run_pairs(lists, offsets, own, far, before)
    got_zero, got_one = across(sent_zero, 1), across(sent_one, 3)
    last_zero = across(kept_zero[QUARTER:] + got_zero[QUARTER:], 3)
    last_one = across(kept_one[QUARTER:] + got_one[QUARTER:], 1)
    settled = settle(offsets, (kept_zero, got_zero, last_zero, kept_one, got_one, last_one))
    pieces = [settled[2]]
    for later in range(1, SLABS):
        route = [(i, (i + later) % groups) for i in range(groups)]
        pieces.append(lax.ppermute(settled[2 + later], "orb", route))
    gathered = gather_pair(settled[0], settled[1])
    forces = assemble(gathered)
    spans = deposit(offsets, pieces)
    gathered = gather_pair(*spans)
    slab = merge(gathered)
    return (forces, slab)


def solution(mesh):
    in_specs = (P("orb", None, None), P(("orb", "rep"), None), P())
    out_specs = (P("orb", None, None), P("orb", None))
    return jax.shard_map(shards, mesh=mesh, in_specs=in_specs, out_specs=out_specs, check_vma=False)
```

```python
import functools

import jax
import jax.numpy as jnp
import numpy as np
from jax import lax
from jax.experimental import pallas as pl
from jax.experimental.pallas import tpu as pltpu
from jax.sharding import PartitionSpec as P


BOX = 64
SLAB = 16
WIDE = 96
ITERS = 5
SCREEN = 6.1
LANES = 128
COLS = BOX * BOX // LANES
FRONT = 16
GROUP = 16
ROOM = 32
HALF = COLS // 8
SIDES = (1, 3)
QUARTER = COLS // 4
SLABS = BOX // SLAB + 1
SPAN = WIDE * BOX // 4 + 32 * WIDE
PAIRS_VMEM = 32 * 1024 * 1024
SMALL_VMEM = 12 * 1024 * 1024
SMEM = pl.BlockSpec(memory_space=pltpu.SMEM)
VMEM = pl.BlockSpec(memory_space=pltpu.VMEM)
HBM = pl.BlockSpec(memory_space=pltpu.HBM)


def place():
    return lax.axis_index("orb"), lax.axis_index("rep")


def neighbours(group):
    return group ^ 1, group + 2 * (group & 1) - 1


def lane_of(rows):
    return lax.broadcasted_iota(jnp.int32, (rows, LANES), 1)


def fold(block):
    return jnp.sum(block.reshape(BOX // 8, 8, LANES), axis=0)


def total(partial):
    return jnp.sum(jnp.sum(partial, axis=1, keepdims=True), axis=0, keepdims=True)


def shift_reader(buffer, dz, dx, dy):
    lanes = lane_of(BOX)
    flat = dx * BOX + dy
    blocks = flat >> 7
    turn = flat & (LANES - 1)
    ypos = lanes & (BOX - 1)
    inside = (ypos >= dy) & (ypos < BOX + dy)
    early = lanes < LANES - turn

    def read(c):
        near = buffer[c - blocks + FRONT, pl.ds(ROOM - dz, BOX), :]
        before = buffer[c - blocks + FRONT - 1, pl.ds(ROOM - dz, BOX), :]
        turned = pltpu.roll(jnp.where(early, near, before), turn, 1)
        return jnp.where(inside, turned, 0.0)

    return read


def beside(field, c, center, after, within):
    above = field[c + 1, pl.ds(9, BOX), :]
    below = field[c + 1, pl.ds(7, BOX), :]
    ahead = field[c, pl.ds(8, BOX), :]
    across = pltpu.roll(jnp.where(lane_of(BOX) < BOX, after, ahead), BOX, 1)
    high = center.astype(jnp.bfloat16)
    low = (center - high.astype(jnp.float32)).astype(jnp.bfloat16)
    inner = jnp.dot(jnp.concatenate([high, low], axis=1), within[...], preferred_element_type=jnp.float32)
    return (inner + across) + (above + below)


def columns(c):
    return pl.ds(pl.multiple_of(c * LANES, LANES), LANES)


def load_box(own, other, which, write):
    for boxes, first in ((own, 0), (other, 2)):

        @pl.when((which >= first) & (which < first + 2))
        def _():
            def block(c, carry):
                write(c, boxes[which - first, :, columns(c)])
                return carry

            lax.fori_loop(0, COLS, block, 0, unroll=8)


def solve_pair(own, other, first, second, delta, within, buffer, still, shifted, basis, image):
    def to_buffer(c, block):
        buffer[c + FRONT, pl.ds(ROOM, BOX), :] = block

    def to_still(c, block):
        still[c] = block

    load_box(own, other, first, to_buffer)
    load_box(own, other, second, to_still)
    read = shift_reader(buffer, *delta)
    diagonal, coupling = [], []
    norm_before = None
    for k in range(ITERS):
        field = basis.at[k]

        def value_of(c):
            if k == 0:
                moved = read(c)
                shifted[c] = moved
                return still[c] * moved
            fresh = image[c] - diagonal[k - 1] * basis[k - 1, c + 1, pl.ds(8, BOX), :]
            if k > 1:
                fresh = fresh - coupling[k - 1] * basis[k - 2, c + 1, pl.ds(8, BOX), :]
            return fresh

        def group(m, carry):
            norm, cross = carry
            start = m * GROUP
            values = [field[start + 1, pl.ds(8, BOX), :]]
            for u in range(1, GROUP + 1):
                if u < GROUP:
                    fresh = value_of(start + u)
                else:
                    fresh = jnp.where(start + u < COLS, value_of(jnp.minimum(start + u, COLS - 1)), 0.0)
                field[start + u + 1, pl.ds(8, BOX), :] = fresh
                norm = norm + fold(fresh * fresh)
                values.append(fresh)
            for u in range(GROUP):
                result = beside(field, start + u, values[u], values[u + 1], within)
                if k < ITERS - 1:
                    image[start + u] = result
                cross = cross + fold(values[u] * result)
            return norm, cross

        opening = value_of(0)
        field[1, pl.ds(8, BOX), :] = opening
        carry = (fold(opening * opening), jnp.zeros((8, LANES), jnp.float32))
        norm, cross = lax.fori_loop(0, COLS // GROUP, group, carry)
        norm = total(norm)
        diagonal.append(total(cross) / norm)
        coupling.append(norm / norm_before if k > 0 else None)
        norm_before = norm
    pivots = [SCREEN - diagonal[0]]
    rights = [jnp.ones_like(pivots[0])]
    for k in range(1, ITERS):
        pivots.append(SCREEN - diagonal[k] - coupling[k] / pivots[k - 1])
        rights.append(rights[k - 1] / pivots[k - 1])
    weights = [None] * ITERS
    weights[ITERS - 1] = rights[ITERS - 1] / pivots[ITERS - 1]
    for k in range(ITERS - 2, -1, -1):
        weights[k] = (rights[k] + coupling[k + 1] * weights[k + 1]) / pivots[k]
    return weights


def run_pair(boxes, targets, within, forces, *scratch):
    buffer, still, shifted, basis, image = scratch
    delta = boxes[4]
    first, second, to_first, to_second = targets
    weights = solve_pair(*boxes, within, *scratch)

    def finish(c, carry):
        potential = weights[0] * basis[0, c + 1, pl.ds(8, BOX), :]
        for k in range(1, ITERS):
            potential = potential + weights[k] * basis[k, c + 1, pl.ds(8, BOX), :]
        image[c] = potential
        buffer[c + FRONT, pl.ds(ROOM, BOX), :] = potential * still[c]
        return carry

    lax.fori_loop(0, COLS, finish, 0, unroll=4)

    @pl.when(to_second)
    def _():
        def deposit(c, carry):
            forces[second, c] = forces[second, c] + image[c] * shifted[c]
            return carry

        lax.fori_loop(0, COLS, deposit, 0, unroll=4)

    @pl.when(to_first)
    def _():
        read = shift_reader(buffer, -delta[0], -delta[1], -delta[2])

        def deposit(c, carry):
            forces[first, c] = forces[first, c] + read(c)
            return carry

        lax.fori_loop(0, COLS, deposit, 0, unroll=8)


def pairs_kernel(phase, faraway, held, *refs):
    begun = phase > 0 or faraway
    lists, offsets, own, other_far, within, *refs = refs
    if begun:
        tally, forces_in, *refs = refs
    other, other_sem, *scratch = refs[-7:]
    buffer, basis = scratch[0], scratch[3]
    if faraway:
        *parts, tally_out, forces = refs[:6]
    else:
        forces, tally_out = refs[:2]
    group, mine = place()
    near, far = neighbours(group)
    neighbour, which = (far, 2) if faraway else (near, 1)
    copy = pltpu.make_async_copy(other_far, other, other_sem)
    copy.start()

    def clear(c, carry):
        buffer[c] = jnp.zeros((BOX + 2 * ROOM, LANES), jnp.float32)
        return carry

    lax.fori_loop(0, COLS + 2 * FRONT, clear, 0, unroll=4)
    nothing = jnp.zeros((BOX + 16, LANES), jnp.float32)
    for k in range(ITERS):
        basis[k, 0] = nothing

        def clear_ends(c, carry):
            basis[k, c + 1, pl.ds(0, 8), :] = jnp.zeros((8, LANES), jnp.float32)
            basis[k, c + 1, pl.ds(BOX + 8, 8), :] = jnp.zeros((8, LANES), jnp.float32)
            return carry

        lax.fori_loop(0, COLS, clear_ends, 0, unroll=4)

    def open_forces(c, carry):
        for k in held:
            block = jnp.zeros((BOX, LANES), jnp.float32)
            if begun:
                block = forces_in[k if forces_in.shape[0] > 1 else 0, c]
            forces[k - held[0], c] = block
        return carry

    lax.fori_loop(0, COLS, open_forces, 0, unroll=2)
    copy.wait()

    def slot(n, count):
        foreign = n >> 4
        row = n & 15
        base = ((row >> 2) ^ mine) * 36 + foreign * (which * 12) + (row & 3) * 3
        first = lists[base]
        second = lists[base + 1]
        live = lists[base + 2] > 0
        second_group = second >> 1
        inner = second_group == group
        outer = second_group == neighbour
        second_at = second - 2 * group
        first_at = first - 2 * group
        if faraway:
            wanted = jnp.where(foreign > 0, inner, outer)
        else:
            wanted = jnp.where(foreign > 0, inner, inner | outer)
        if phase == 0:
            timely = ((foreign == 0) & (first_at == 0)) | (inner & (second_at == 0))
        else:
            timely = ((foreign > 0) | (first_at == 1)) & (jnp.logical_not(inner) | (second_at == 1))
        taken = live & wanted & timely
        turn = taken & ((count & 3) == mine)

        @pl.when(turn)
        def _():
            delta = [offsets[first * 3 + axis] - offsets[second * 3 + axis] for axis in range(3)]
            first_box = jnp.where(foreign > 0, 2 + first - 2 * neighbour, first_at)
            second_box = jnp.where(inner, second_at, 2 + second - 2 * neighbour)
            boxes = (own, other, first_box, second_box, delta)
            targets = (first_at - held[0], second_at - held[0], foreign == 0, inner)
            run_pair(boxes, targets, within, forces, *scratch)

        return count + taken.astype(jnp.int32)

    tally_out[0] = lax.fori_loop(0, 32, slot, tally[0] if begun else jnp.int32(0))
    if not faraway:
        return
    for h, side in enumerate(SIDES):
        for n, who in enumerate((mine ^ side, mine)):
            for m, quarter in enumerate((who, who ^ (4 - side))):
                for c in range(HALF):
                    parts[2 * h + n][m * HALF + c] = forces[0, quarter * QUARTER + h * HALF + c]


def within_block():
    lane = np.arange(LANES)
    gap = np.abs(lane[:, None] - lane[None, :])
    same_row = lane[:, None] // BOX == lane[None, :] // BOX
    once = ((gap == 1) & same_row) | (gap == BOX)
    return jnp.asarray(np.concatenate([once, once]), jnp.bfloat16)


def stage_kernel(boxes, out):
    pltpu.sync_copy(boxes, out)


def stage(boxes):
    return pl.pallas_call(
        stage_kernel,
        out_shape=jax.ShapeDtypeStruct(boxes.shape, boxes.dtype),
        in_specs=[HBM],
        out_specs=VMEM,
        compiler_params=pltpu.CompilerParams(vmem_limit_bytes=SMALL_VMEM),
        cost_estimate=pl.CostEstimate(flops=1_000_000, bytes_accessed=4 << 20, transcendentals=0),
        name="stage",
    )(boxes)


def run_pairs(lists, offsets, own, other, phase, faraway, tally=None, forces=None):
    operands = [lists, offsets, own, other, within_block()]
    in_specs = [SMEM, SMEM, VMEM, HBM, VMEM]
    held = (0, 1) if tally is None else (phase,)
    whole = (len(held), COLS, BOX, LANES)
    scratch = [
        pltpu.VMEM((2, BOX, BOX * BOX), jnp.float32),
        pltpu.SemaphoreType.DMA,
        pltpu.VMEM((COLS + 2 * FRONT, BOX + 2 * ROOM, LANES), jnp.float32),
        pltpu.VMEM((COLS, BOX, LANES), jnp.float32),
        pltpu.VMEM((COLS, BOX, LANES), jnp.float32),
        pltpu.VMEM((ITERS, COLS + 2, BOX + 16, LANES), jnp.float32),
        pltpu.VMEM((COLS, BOX, LANES), jnp.float32),
    ]
    if tally is not None:
        operands += [tally, forces]
        in_specs += [SMEM, VMEM]
    counted = jax.ShapeDtypeStruct((1,), jnp.int32)
    if faraway:
        out_shape = [jax.ShapeDtypeStruct((2 * HALF, BOX, LANES), jnp.float32)] * 4 + [counted]
        out_specs = [VMEM] * 4 + [SMEM]
        scratch = [pltpu.VMEM(whole, jnp.float32)] + scratch
    else:
        out_shape = [jax.ShapeDtypeStruct(whole, jnp.float32), counted]
        out_specs = [VMEM, SMEM]
    return pl.pallas_call(
        functools.partial(pairs_kernel, phase, faraway, held),
        out_shape=out_shape,
        in_specs=in_specs,
        out_specs=out_specs,
        scratch_shapes=scratch,
        compiler_params=pltpu.CompilerParams(vmem_limit_bytes=PAIRS_VMEM),
        cost_estimate=pl.CostEstimate(flops=100_000_000, bytes_accessed=8 << 20, transcendentals=0),
    )(*operands)


def settle_kernel(phase, offsets, *refs):
    parts, refs = refs[:6], refs[6:]
    if phase > 0:
        earlier, refs = refs[:2], refs[2:]
    sums, pieces, tall = refs[:2], refs[2 : 2 + SLABS], refs[-1]
    group, _ = place()
    tall[:, pl.ds(0, SLAB), :] = jnp.zeros((QUARTER, SLAB, LANES), jnp.float32)
    tall[:, pl.ds(SLAB + BOX, SLAB), :] = jnp.zeros((QUARTER, SLAB, LANES), jnp.float32)
    for h in range(2):
        kept, once, twice = parts[3 * h : 3 * h + 3]
        for c in range(HALF):
            value = (kept[c] + once[c]) + twice[c]
            if phase > 0:
                sums[h][0, c] = earlier[h][0, c]
            sums[h][phase, c] = value
            tall[h * HALF + c, pl.ds(SLAB, BOX), :] = value
    depth = offsets[(2 * group + phase) * 3] - group * SLAB
    for t in range(SLABS):
        for c in range(QUARTER):
            pieces[t][c] = tall[c, pl.ds(SLAB * (t + 1) - depth, SLAB), :]


def settle(offsets, phase, parts, earlier=()):
    half = jax.ShapeDtypeStruct((phase + 1, HALF, BOX, LANES), jnp.float32)
    piece = jax.ShapeDtypeStruct((QUARTER, SLAB, LANES), jnp.float32)
    return pl.pallas_call(
        functools.partial(settle_kernel, phase),
        out_shape=[half] * 2 + [piece] * SLABS,
        in_specs=[SMEM] + [VMEM] * (6 + len(earlier)),
        out_specs=[VMEM] * (2 + SLABS),
        scratch_shapes=[pltpu.VMEM((QUARTER, BOX + 2 * SLAB, LANES), jnp.float32)],
        compiler_params=pltpu.CompilerParams(vmem_limit_bytes=SMALL_VMEM),
        cost_estimate=pl.CostEstimate(flops=4_000_000, bytes_accessed=4 << 20, transcendentals=0),
    )(offsets, *parts, *earlier)


def deposit_kernel(offsets, *refs):
    pieces, outs, table, span = refs[: 2 * SLABS], refs[2 * SLABS : 2 * SLABS + 2], refs[-2], refs[-1]
    group, _ = place()
    groups = lax.axis_size("orb")
    lanes = lax.broadcasted_iota(jnp.int32, (SLAB, LANES), 1)
    span[...] = jnp.zeros_like(span)
    for n in range(2 * SLABS):
        table[n] = pieces[n][...]

    def lay(n, carry):
        k = (n >= SLABS).astype(jnp.int32)
        owner = (group + groups - (n - k * SLABS)) & (groups - 1)
        at = (2 * owner + k) * 3
        base = offsets[at + 1] * WIDE + offsets[at + 2]
        for c in range(QUARTER):
            value = table[n, c]
            for row in range(2):
                start = base + (2 * c + row) * WIDE - row * BOX
                tile, turn = start >> 7, start & (LANES - 1)
                kept = (lanes < BOX) if row == 0 else (lanes >= BOX)
                turned = pltpu.roll(jnp.where(kept, value, 0.0), turn, 1)
                here = pl.ds(pl.multiple_of(tile * LANES, LANES), LANES)
                there = pl.ds(pl.multiple_of(tile * LANES + LANES, LANES), LANES)
                span[:, here] = span[:, here] + jnp.where(lanes >= turn, turned, 0.0)
                span[:, there] = span[:, there] + jnp.where(lanes < turn, turned, 0.0)
        return carry

    lax.fori_loop(0, 2 * SLABS, lay, 0)
    for half in range(2):
        outs[half][...] = span[pl.ds(8 * half, 8), pl.ds(0, SPAN)]


def deposit(offsets, pieces):
    half = jax.ShapeDtypeStruct((SLAB // 2, SPAN), jnp.float32)
    return pl.pallas_call(
        deposit_kernel,
        out_shape=[half] * 2,
        in_specs=[SMEM] + [VMEM] * (2 * SLABS),
        out_specs=[VMEM] * 2,
        scratch_shapes=[
            pltpu.VMEM((2 * SLABS, QUARTER, SLAB, LANES), jnp.float32),
            pltpu.VMEM((SLAB, SPAN + 4 * LANES), jnp.float32),
        ],
        cost_estimate=pl.CostEstimate(flops=8_000_000, bytes_accessed=2 << 20, transcendentals=0),
        compiler_params=pltpu.CompilerParams(vmem_limit_bytes=SMALL_VMEM),
        name="deposit",
    )(offsets, *pieces)


def quarters_of(mine):
    return mine, mine ^ 1, mine ^ 3, mine ^ 2


def merge_kernel(*refs):
    spans, out = refs[:8], refs[8]
    _, mine = place()
    out[...] = jnp.zeros_like(out)
    for n, quarter in enumerate(quarters_of(mine)):
        where = pl.ds(pl.multiple_of(quarter * (WIDE * BOX // 4), LANES), SPAN)
        for half in range(2):
            rows = pl.ds(8 * half, 8)
            out[rows, where] = out[rows, where] + spans[2 * n + half][...]


def merge(spans):
    return pl.pallas_call(
        merge_kernel,
        out_shape=jax.ShapeDtypeStruct((SLAB, WIDE * WIDE), jnp.float32),
        in_specs=[VMEM] * 8,
        out_specs=VMEM,
        cost_estimate=pl.CostEstimate(flops=1_000_000, bytes_accessed=2 << 20, transcendentals=0),
        compiler_params=pltpu.CompilerParams(vmem_limit_bytes=SMALL_VMEM),
        name="merge",
    )(*spans)


def assemble_kernel(*refs):
    parts, out = refs[:8], refs[8]
    _, mine = place()
    for n, quarter in enumerate(quarters_of(mine)):
        for h in range(2):
            for c in range(HALF):
                where = pl.ds(pl.multiple_of((quarter * QUARTER + h * HALF + c) * LANES, LANES), LANES)
                for k in range(2):
                    out[k, :, where] = parts[2 * n + h][k, c]


def assemble(parts):
    return pl.pallas_call(
        assemble_kernel,
        out_shape=jax.ShapeDtypeStruct((2, BOX, BOX * BOX), jnp.float32),
        in_specs=[VMEM] * 8,
        out_specs=VMEM,
        cost_estimate=pl.CostEstimate(flops=1_000_000, bytes_accessed=4 << 20, transcendentals=0),
        compiler_params=pltpu.CompilerParams(vmem_limit_bytes=SMALL_VMEM),
        name="assemble",
    )(*parts)


def across(block, side):
    return lax.ppermute(block, "rep", [(i, i ^ side) for i in range(lax.axis_size("rep"))])


def gather_pair(first, second):
    first_one, first_three = across(first, 1), across(first, 3)
    second_one, second_three = across(second, 1), across(second, 3)
    first_two = across(first_three, 1)
    second_two = across(second_one, 3)
    return [first, second, first_one, second_one, first_three, second_three, first_two, second_two]


def reduce_scatter(parts):
    sent, kept = parts[0::2], parts[1::2]
    got = [across(sent[h], side) for h, side in enumerate(SIDES)]
    passed = [kept[h][HALF:] + got[h][HALF:] for h in range(2)]
    last = [across(passed[h], 4 - side) for h, side in enumerate(SIDES)]
    return [kept[0], got[0], last[0], kept[1], got[1], last[1]]


def deal(pieces, groups):
    dealt = [pieces[0]]
    for later in range(1, SLABS):
        dealt.append(lax.ppermute(pieces[later], "orb", [(i, (i + later) % groups) for i in range(groups)]))
    return dealt


def shards(orbitals, pair_list, box_offsets):
    groups = lax.axis_size("orb")
    to_near = [(g, g ^ 1) for g in range(groups)]
    to_far = [(g, neighbours(g)[1]) for g in range(groups) if 0 <= neighbours(g)[1] < groups]
    slots = pair_list.reshape(-1)
    near_slots = lax.ppermute(slots, "orb", to_near)
    far_slots = lax.ppermute(slots, "orb", to_far)
    near = lax.ppermute(orbitals, "orb", to_near)
    far = lax.ppermute(orbitals, "orb", to_far)
    known = jnp.concatenate([slots, near_slots, far_slots])
    lists = jnp.concatenate([known] + [across(known, side) for side in (1, 2, 3)])
    offsets = box_offsets.reshape(-1)
    own = stage(orbitals)
    shared, tally = run_pairs(lists, offsets, own, near, 0, False)
    *parts, tally = run_pairs(lists, offsets, own, far, 0, True, tally, shared)
    summed = reduce_scatter(parts)
    shared, tally = run_pairs(lists, offsets, own, near, 1, False, tally, shared)
    *parts, tally = run_pairs(lists, offsets, own, far, 1, True, tally, shared)
    settled = settle(offsets, 0, summed)
    pieces = deal(settled[2:], groups)
    summed = reduce_scatter(parts)
    settled = settle(offsets, 1, summed, settled[:2])
    pieces += deal(settled[2:], groups)
    gathered = gather_pair(settled[0], settled[1])
    forces = assemble(gathered)
    spans = deposit(offsets, pieces)
    gathered = gather_pair(*spans)
    slab = merge(gathered)
    return (forces, slab)


def solution(mesh):
    in_specs = (P("orb", None, None), P(("orb", "rep"), None), P())
    out_specs = (P("orb", None, None), P("orb", None))
    return jax.shard_map(shards, mesh=mesh, in_specs=in_specs, out_specs=out_specs, check_vma=False)
```

```python
import functools

import jax
import jax.numpy as jnp
import numpy as np
from jax import lax
from jax.experimental import pallas as pl
from jax.experimental.pallas import tpu as pltpu
from jax.sharding import PartitionSpec as P


BOX = 64
SLAB = 16
WIDE = 96
ITERS = 5
SCREEN = 6.1
LANES = 128
COLS = BOX * BOX // LANES
FRONT = 16
GROUP = 16
ROOM = 32
QUARTER = COLS // 4
SLABS = BOX // SLAB + 1
SPAN = WIDE * BOX // 4 + 32 * WIDE
PAIRS_VMEM = 32 * 1024 * 1024
SMALL_VMEM = 12 * 1024 * 1024
SMEM = pl.BlockSpec(memory_space=pltpu.SMEM)
VMEM = pl.BlockSpec(memory_space=pltpu.VMEM)
HBM = pl.BlockSpec(memory_space=pltpu.HBM)


def place():
    return lax.axis_index("orb"), lax.axis_index("rep")


def neighbours(group):
    return group ^ 1, group + 2 * (group & 1) - 1


def lane_of(rows):
    return lax.broadcasted_iota(jnp.int32, (rows, LANES), 1)


def fold(block):
    return jnp.sum(block.reshape(BOX // 8, 8, LANES), axis=0)


def total(partial):
    return jnp.sum(jnp.sum(partial, axis=1, keepdims=True), axis=0, keepdims=True)


def shift_reader(buffer, dz, dx, dy):
    lanes = lane_of(BOX)
    flat = dx * BOX + dy
    blocks = flat >> 7
    turn = flat & (LANES - 1)
    ypos = lanes & (BOX - 1)
    inside = (ypos >= dy) & (ypos < BOX + dy)
    early = lanes < LANES - turn

    def read(c):
        near = buffer[c - blocks + FRONT, pl.ds(ROOM - dz, BOX), :]
        before = buffer[c - blocks + FRONT - 1, pl.ds(ROOM - dz, BOX), :]
        turned = pltpu.roll(jnp.where(early, near, before), turn, 1)
        return jnp.where(inside, turned, 0.0)

    return read


def beside(field, c, center, after, within):
    above = field[c + 1, pl.ds(9, BOX), :]
    below = field[c + 1, pl.ds(7, BOX), :]
    ahead = field[c, pl.ds(8, BOX), :]
    across = pltpu.roll(jnp.where(lane_of(BOX) < BOX, after, ahead), BOX, 1)
    high = center.astype(jnp.bfloat16)
    low = (center - high.astype(jnp.float32)).astype(jnp.bfloat16)
    inner = jnp.dot(jnp.concatenate([high, low], axis=1), within[...], preferred_element_type=jnp.float32)
    return (inner + across) + (above + below)


def columns(c):
    return pl.ds(pl.multiple_of(c * LANES, LANES), LANES)


def load_box(groups, which, write):
    for n, boxes in enumerate(groups):
        first = 2 * n

        @pl.when((which >= first) & (which < first + 2))
        def _():
            def block(c, carry):
                write(c, boxes[which - first, :, columns(c)])
                return carry

            lax.fori_loop(0, COLS, block, 0, unroll=8)


def solve_pair(groups, first, second, delta, within, buffer, still, shifted, basis, image):
    def to_buffer(c, block):
        buffer[c + FRONT, pl.ds(ROOM, BOX), :] = block

    def to_still(c, block):
        still[c] = block

    load_box(groups, first, to_buffer)
    load_box(groups, second, to_still)
    read = shift_reader(buffer, *delta)
    diagonal, coupling = [], []
    norm_before = None
    for k in range(ITERS):
        field = basis.at[k]

        def value_of(c):
            if k == 0:
                moved = read(c)
                shifted[c] = moved
                return still[c] * moved
            fresh = image[c] - diagonal[k - 1] * basis[k - 1, c + 1, pl.ds(8, BOX), :]
            if k > 1:
                fresh = fresh - coupling[k - 1] * basis[k - 2, c + 1, pl.ds(8, BOX), :]
            return fresh

        def group(start, carry, final):
            norm, cross = carry
            center = field[start + 1, pl.ds(8, BOX), :]
            values = [center]
            for u in range(1, GROUP + 1):
                if final and u == GROUP:
                    values.append(jnp.zeros_like(center))
                    continue
                fresh = value_of(start + u)
                field[start + u + 1, pl.ds(8, BOX), :] = fresh
                norm = norm + fold(fresh * fresh)
                values.append(fresh)
            for u in range(GROUP):
                result = beside(field, start + u, values[u], values[u + 1], within)
                if k < ITERS - 1:
                    image[start + u] = result
                cross = cross + fold(values[u] * result)
            return norm, cross

        opening = value_of(0)
        field[1, pl.ds(8, BOX), :] = opening
        carry = (fold(opening * opening), jnp.zeros((8, LANES), jnp.float32))
        carry = lax.fori_loop(0, COLS // GROUP - 1, lambda m, held: group(m * GROUP, held, False), carry)
        norm, cross = group(COLS - GROUP, carry, True)
        norm = total(norm)
        diagonal.append(total(cross) / norm)
        coupling.append(norm / norm_before if k > 0 else None)
        norm_before = norm
    pivots = [SCREEN - diagonal[0]]
    rights = [jnp.ones_like(pivots[0])]
    for k in range(1, ITERS):
        pivots.append(SCREEN - diagonal[k] - coupling[k] / pivots[k - 1])
        rights.append(rights[k - 1] / pivots[k - 1])
    weights = [None] * ITERS
    weights[ITERS - 1] = rights[ITERS - 1] / pivots[ITERS - 1]
    for k in range(ITERS - 2, -1, -1):
        weights[k] = (rights[k] + coupling[k + 1] * weights[k + 1]) / pivots[k]
    return weights


def run_pair(groups, first, second, delta, to_second, to_first, within, forces, *scratch):
    buffer, still, shifted, basis, image = scratch
    weights = solve_pair(groups, first, second, delta, within, *scratch)

    def finish(c, carry):
        potential = weights[0] * basis[0, c + 1, pl.ds(8, BOX), :]
        for k in range(1, ITERS):
            potential = potential + weights[k] * basis[k, c + 1, pl.ds(8, BOX), :]
        image[c] = potential
        buffer[c + FRONT, pl.ds(ROOM, BOX), :] = potential * still[c]
        return carry

    lax.fori_loop(0, COLS, finish, 0, unroll=4)

    @pl.when(to_second)
    def _():
        def deposit(c, carry):
            forces[second, c] = forces[second, c] + image[c] * shifted[c]
            return carry

        lax.fori_loop(0, COLS, deposit, 0, unroll=4)

    @pl.when(to_first)
    def _():
        read = shift_reader(buffer, -delta[0], -delta[1], -delta[2])

        def deposit(c, carry):
            forces[first, c] = forces[first, c] + read(c)
            return carry

        lax.fori_loop(0, COLS, deposit, 0, unroll=8)


def pairs_kernel(begun, *refs):
    lists, refs = refs[: 3 if begun else 1], refs[3 if begun else 1 :]
    offsets, own, *far_away = refs[: 4 if begun else 3]
    refs = refs[2 + len(far_away) :]
    if begun:
        within, tally, forces_in, *parts, forces = refs[:8]
    else:
        within, forces, tally_out = refs[:3]
    arrived, arrival_sems, table, *scratch = refs[-8:]
    buffer, basis = scratch[0], scratch[3]
    group, mine = place()
    near, far = neighbours(group)
    boxes = [own] + [arrived.at[n] for n in range(len(far_away))]
    copies = [pltpu.make_async_copy(f, boxes[n + 1], arrival_sems.at[n]) for n, f in enumerate(far_away)]
    for copy in copies:
        copy.start()

    def clear(c, carry):
        buffer[c] = jnp.zeros((BOX + 2 * ROOM, LANES), jnp.float32)
        return carry

    lax.fori_loop(0, COLS + 2 * FRONT, clear, 0, unroll=4)
    nothing = jnp.zeros((BOX + 16, LANES), jnp.float32)
    for k in range(ITERS):
        basis[k, 0] = nothing

        def clear_ends(c, carry):
            basis[k, c + 1, pl.ds(0, 8), :] = jnp.zeros((8, LANES), jnp.float32)
            basis[k, c + 1, pl.ds(BOX + 8, 8), :] = jnp.zeros((8, LANES), jnp.float32)
            return carry

        lax.fori_loop(0, COLS, clear_ends, 0, unroll=4)

    def open_forces(c, carry):
        for k in range(2):
            forces[k, c] = forces_in[k, c] if begun else jnp.zeros((BOX, LANES), jnp.float32)
        return carry

    lax.fori_loop(0, COLS, open_forces, 0, unroll=2)

    def scan_list(n, slots, carry):
        def scan(row, carry):
            count, found = carry
            base = ((row >> 2) ^ mine) * 12 + (row & 3) * 3
            first, second, live = slots[base], slots[base + 1], slots[base + 2]
            second_group = second >> 1
            if n > 0:
                wanted = second_group == group
            elif begun:
                wanted = second_group == far
            else:
                wanted = (second_group == group) | (second_group == near)
            taken = (live > 0) & wanted
            table[3 * found] = n
            table[3 * found + 1] = first
            table[3 * found + 2] = second
            found = found + (taken & ((count & 3) == mine)).astype(jnp.int32)
            return count + taken.astype(jnp.int32), found

        return lax.fori_loop(0, 16, scan, carry, unroll=4)

    carry = (tally[0] if begun else jnp.int32(0), jnp.int32(0))
    for n, slots in enumerate(lists):
        carry = scan_list(n, slots, carry)
    count, found = carry
    for copy in copies:
        copy.wait()

    def pair(m, carry):
        home, first, second = table[3 * m], table[3 * m + 1], table[3 * m + 2]
        delta = [offsets[first * 3 + axis] - offsets[second * 3 + axis] for axis in range(3)]

        def box_of(orbital):
            base = jnp.where((orbital >> 1) == group, group, jnp.where((orbital >> 1) == near, near - 1, far - 2))
            return orbital - 2 * base

        run_pair(boxes, box_of(first), box_of(second), delta, (second >> 1) == group, home == 0, within, forces, *scratch)
        return carry

    lax.fori_loop(0, found, pair, 0)
    if not begun:
        tally_out[0] = count
        return
    for k, side in enumerate((1, 3)):
        for n, who in enumerate((mine ^ side, mine)):
            for half, quarter in enumerate((who, who ^ (4 - side))):
                for c in range(QUARTER):
                    parts[2 * k + n][half * QUARTER + c] = forces[k, quarter * QUARTER + c]


def within_block():
    lane = np.arange(LANES)
    gap = np.abs(lane[:, None] - lane[None, :])
    same_row = lane[:, None] // BOX == lane[None, :] // BOX
    once = ((gap == 1) & same_row) | (gap == BOX)
    return jnp.asarray(np.concatenate([once, once]), jnp.bfloat16)


def stage_kernel(boxes, out):
    pltpu.sync_copy(boxes, out)


def stage(boxes):
    return pl.pallas_call(
        stage_kernel,
        out_shape=jax.ShapeDtypeStruct(boxes.shape, boxes.dtype),
        in_specs=[HBM],
        out_specs=VMEM,
        compiler_params=pltpu.CompilerParams(vmem_limit_bytes=SMALL_VMEM),
        cost_estimate=pl.CostEstimate(flops=1_000_000, bytes_accessed=4 << 20, transcendentals=0),
        name="stage",
    )(boxes)


def run_pairs(lists, offsets, own, others, before=None):
    begun = before is not None
    operands = [*lists, offsets, own, *others, within_block()]
    in_specs = [SMEM] * (len(lists) + 1) + [VMEM] + [HBM] * len(others) + [VMEM]
    whole = (2, COLS, BOX, LANES)
    scratch = [
        pltpu.VMEM((len(others), 2, BOX, BOX * BOX), jnp.float32),
        pltpu.SemaphoreType.DMA((len(others),)),
        pltpu.SMEM((3 * 64,), jnp.int32),
        pltpu.VMEM((COLS + 2 * FRONT, BOX + 2 * ROOM, LANES), jnp.float32),
        pltpu.VMEM((COLS, BOX, LANES), jnp.float32),
        pltpu.VMEM((COLS, BOX, LANES), jnp.float32),
        pltpu.VMEM((ITERS, COLS + 1, BOX + 16, LANES), jnp.float32),
        pltpu.VMEM((COLS, BOX, LANES), jnp.float32),
    ]
    if begun:
        operands += [before[1], before[0]]
        in_specs += [SMEM, VMEM]
        out_shape = [jax.ShapeDtypeStruct((2 * QUARTER, BOX, LANES), jnp.float32)] * 4
        out_specs = [VMEM] * 4
        scratch = [pltpu.VMEM(whole, jnp.float32)] + scratch
    else:
        out_shape = [jax.ShapeDtypeStruct(whole, jnp.float32), jax.ShapeDtypeStruct((1,), jnp.int32)]
        out_specs = [VMEM, SMEM]
    return pl.pallas_call(
        functools.partial(pairs_kernel, begun),
        out_shape=out_shape,
        in_specs=in_specs,
        out_specs=out_specs,
        scratch_shapes=scratch,
        compiler_params=pltpu.CompilerParams(vmem_limit_bytes=PAIRS_VMEM),
        cost_estimate=pl.CostEstimate(flops=100_000_000, bytes_accessed=8 << 20, transcendentals=0),
        name="pairs_far" if begun else "pairs_near",
    )(*operands)


def settle_kernel(offsets, *refs):
    parts, sums, pieces, tall = refs[:6], refs[6:8], refs[8:13], refs[13]
    group, _ = place()
    for k in range(2):
        kept, once, twice = parts[3 * k : 3 * k + 3]
        tall[:, pl.ds(0, SLAB), :] = jnp.zeros((QUARTER, SLAB, LANES), jnp.float32)
        tall[:, pl.ds(SLAB + BOX, SLAB), :] = jnp.zeros((QUARTER, SLAB, LANES), jnp.float32)
        for c in range(QUARTER):
            value = (kept[c] + once[c]) + twice[c]
            sums[k][c] = value
            tall[c, pl.ds(SLAB, BOX), :] = value
        depth = offsets[(2 * group + k) * 3] - group * SLAB
        for t in range(SLABS):
            for c in range(QUARTER):
                pieces[t][k, c] = tall[c, pl.ds(SLAB * (t + 1) - depth, SLAB), :]


def settle(offsets, parts):
    quarter = jax.ShapeDtypeStruct((QUARTER, BOX, LANES), jnp.float32)
    piece = jax.ShapeDtypeStruct((2, QUARTER, SLAB, LANES), jnp.float32)
    return pl.pallas_call(
        settle_kernel,
        out_shape=[quarter] * 2 + [piece] * SLABS,
        in_specs=[SMEM] + [VMEM] * 6,
        out_specs=[VMEM] * (2 + SLABS),
        scratch_shapes=[pltpu.VMEM((QUARTER, BOX + 2 * SLAB, LANES), jnp.float32)],
        cost_estimate=pl.CostEstimate(flops=4_000_000, bytes_accessed=4 << 20, transcendentals=0),
        compiler_params=pltpu.CompilerParams(vmem_limit_bytes=SMALL_VMEM),
        name="settle",
    )(offsets, *parts)


def deposit_kernel(offsets, *refs):
    pieces, outs, span = refs[:SLABS], refs[SLABS : SLABS + 2], refs[-1]
    group, _ = place()
    lanes = lax.broadcasted_iota(jnp.int32, (SLAB, LANES), 1)
    span[...] = jnp.zeros_like(span)
    for t in range(SLABS):
        owner = (group + lax.axis_size("orb") - t) % lax.axis_size("orb")

        def lay(k, carry):
            at = (2 * owner + k) * 3
            base = offsets[at + 1] * WIDE + offsets[at + 2]
            for c in range(QUARTER):
                value = pieces[t][k, c]
                for row in range(2):
                    start = base + (2 * c + row) * WIDE - row * BOX
                    tile, turn = start >> 7, start & (LANES - 1)
                    kept = (lanes < BOX) if row == 0 else (lanes >= BOX)
                    turned = pltpu.roll(jnp.where(kept, value, 0.0), turn, 1)
                    here = pl.ds(pl.multiple_of(tile * LANES, LANES), LANES)
                    there = pl.ds(pl.multiple_of(tile * LANES + LANES, LANES), LANES)
                    span[:, here] = span[:, here] + jnp.where(lanes >= turn, turned, 0.0)
                    span[:, there] = span[:, there] + jnp.where(lanes < turn, turned, 0.0)
            return carry

        lax.fori_loop(0, 2, lay, 0)
    for half in range(2):
        outs[half][...] = span[pl.ds(8 * half, 8), pl.ds(0, SPAN)]


def deposit(offsets, pieces):
    half = jax.ShapeDtypeStruct((SLAB // 2, SPAN), jnp.float32)
    return pl.pallas_call(
        deposit_kernel,
        out_shape=[half] * 2,
        in_specs=[SMEM] + [VMEM] * SLABS,
        out_specs=[VMEM] * 2,
        scratch_shapes=[pltpu.VMEM((SLAB, SPAN + 4 * LANES), jnp.float32)],
        cost_estimate=pl.CostEstimate(flops=8_000_000, bytes_accessed=2 << 20, transcendentals=0),
        compiler_params=pltpu.CompilerParams(vmem_limit_bytes=SMALL_VMEM),
        name="deposit",
    )(offsets, *pieces)


def quarters_of(mine):
    return mine, mine ^ 1, mine ^ 3, mine ^ 2


def merge_kernel(*refs):
    spans, out = refs[:8], refs[8]
    _, mine = place()
    out[...] = jnp.zeros_like(out)
    for n, quarter in enumerate(quarters_of(mine)):
        where = pl.ds(pl.multiple_of(quarter * (WIDE * BOX // 4), LANES), SPAN)
        for half in range(2):
            rows = pl.ds(8 * half, 8)
            out[rows, where] = out[rows, where] + spans[2 * n + half][...]


def merge(spans):
    return pl.pallas_call(
        merge_kernel,
        out_shape=jax.ShapeDtypeStruct((SLAB, WIDE * WIDE), jnp.float32),
        in_specs=[VMEM] * 8,
        out_specs=VMEM,
        cost_estimate=pl.CostEstimate(flops=1_000_000, bytes_accessed=2 << 20, transcendentals=0),
        compiler_params=pltpu.CompilerParams(vmem_limit_bytes=SMALL_VMEM),
        name="merge",
    )(*spans)


def assemble_kernel(*refs):
    parts, out = refs[:8], refs[8]
    _, mine = place()
    for n, quarter in enumerate(quarters_of(mine)):
        for k in range(2):
            for c in range(QUARTER):
                where = pl.ds(pl.multiple_of((quarter * QUARTER + c) * LANES, LANES), LANES)
                out[k, :, where] = parts[2 * n + k][c]


def assemble(parts):
    return pl.pallas_call(
        assemble_kernel,
        out_shape=jax.ShapeDtypeStruct((2, BOX, BOX * BOX), jnp.float32),
        in_specs=[VMEM] * 8,
        out_specs=VMEM,
        cost_estimate=pl.CostEstimate(flops=1_000_000, bytes_accessed=4 << 20, transcendentals=0),
        compiler_params=pltpu.CompilerParams(vmem_limit_bytes=SMALL_VMEM),
        name="assemble",
    )(*parts)


def across(block, side):
    return lax.ppermute(block, "rep", [(i, i ^ side) for i in range(lax.axis_size("rep"))])


def gather_pair(first, second):
    first_three, second_one = across(first, 3), across(second, 1)
    first_one, second_three = across(first, 1), across(second, 3)
    first_two = across(first_three, 1)
    second_two = across(second_one, 3)
    return [first, second, first_one, second_one, first_three, second_three, first_two, second_two]


def shards(orbitals, pair_list, box_offsets):
    groups = lax.axis_size("orb")
    to_near = [(g, g ^ 1) for g in range(groups)]
    to_far = [(g, neighbours(g)[1]) for g in range(groups) if 0 <= neighbours(g)[1] < groups]
    slots = pair_list.reshape(-1)
    known = jnp.concatenate([slots] + [across(slots, side) for side in (1, 2, 3)])
    near = lax.ppermute(orbitals, "orb", to_near)
    far = lax.ppermute(orbitals, "orb", to_far)
    lists = [known, lax.ppermute(known, "orb", to_near), lax.ppermute(known, "orb", to_far)]
    offsets = box_offsets.reshape(-1)
    own = stage(orbitals)
    before = run_pairs(lists[:1], offsets, own, [near])
    sent_zero, kept_zero, sent_one, kept_one = run_pairs(lists, offsets, own, [near, far], before)
    got_zero, got_one = across(sent_zero, 1), across(sent_one, 3)
    last_zero = across(kept_zero[QUARTER:] + got_zero[QUARTER:], 3)
    last_one = across(kept_one[QUARTER:] + got_one[QUARTER:], 1)
    settled = settle(offsets, (kept_zero, got_zero, last_zero, kept_one, got_one, last_one))
    pieces = [settled[2]]
    for later in range(1, SLABS):
        route = [(i, (i + later) % groups) for i in range(groups)]
        pieces.append(lax.ppermute(settled[2 + later], "orb", route))
    gathered = gather_pair(settled[0], settled[1])
    forces = assemble(gathered)
    spans = deposit(offsets, pieces)
    gathered = gather_pair(*spans)
    slab = merge(gathered)
    return (forces, slab)


def solution(mesh):
    in_specs = (P("orb", None, None), P(("orb", "rep"), None), P())
    out_specs = (P("orb", None, None), P("orb", None))
    return jax.shard_map(shards, mesh=mesh, in_specs=in_specs, out_specs=out_specs, check_vma=False)
```

```python
import functools

import jax
import jax.numpy as jnp
import numpy as np
from jax import lax
from jax.experimental import pallas as pl
from jax.experimental.pallas import tpu as pltpu
from jax.sharding import PartitionSpec as P


BOX = 64
SLAB = 16
WIDE = 96
ITERS = 5
SCREEN = 6.1
LANES = 128
COLS = BOX * BOX // LANES
FRONT = 16
GROUP = 16
ROOM = 32
QUARTER = COLS // 4
SLABS = BOX // SLAB + 1
SPAN = WIDE * BOX // 4 + 32 * WIDE
PAIRS_VMEM = 32 * 1024 * 1024
SMALL_VMEM = 12 * 1024 * 1024
SMEM = pl.BlockSpec(memory_space=pltpu.SMEM)
VMEM = pl.BlockSpec(memory_space=pltpu.VMEM)
HBM = pl.BlockSpec(memory_space=pltpu.HBM)


def place():
    return lax.axis_index("orb"), lax.axis_index("rep")


def neighbours(group):
    return group ^ 1, group + 2 * (group & 1) - 1


def lane_of(rows):
    return lax.broadcasted_iota(jnp.int32, (rows, LANES), 1)


def fold(block):
    return jnp.sum(block.reshape(BOX // 8, 8, LANES), axis=0)


def total(partial):
    return jnp.sum(jnp.sum(partial, axis=1, keepdims=True), axis=0, keepdims=True)


def shift_reader(buffer, dz, dx, dy):
    lanes = lane_of(BOX)
    flat = dx * BOX + dy
    blocks = flat >> 7
    turn = flat & (LANES - 1)
    ypos = lanes & (BOX - 1)
    inside = (ypos >= dy) & (ypos < BOX + dy)
    early = lanes < LANES - turn

    def read(c):
        near = buffer[c - blocks + FRONT, pl.ds(ROOM - dz, BOX), :]
        before = buffer[c - blocks + FRONT - 1, pl.ds(ROOM - dz, BOX), :]
        turned = pltpu.roll(jnp.where(early, near, before), turn, 1)
        return jnp.where(inside, turned, 0.0)

    return read


def beside(field, c, center, after, within):
    above = field[c + 1, pl.ds(9, BOX), :]
    below = field[c + 1, pl.ds(7, BOX), :]
    ahead = field[c, pl.ds(8, BOX), :]
    across = pltpu.roll(jnp.where(lane_of(BOX) < BOX, after, ahead), BOX, 1)
    high = center.astype(jnp.bfloat16)
    low = (center - high.astype(jnp.float32)).astype(jnp.bfloat16)
    inner = jnp.dot(jnp.concatenate([high, low], axis=1), within[...], preferred_element_type=jnp.float32)
    return (inner + across) + (above + below)


def columns(c):
    return pl.ds(pl.multiple_of(c * LANES, LANES), LANES)


def load_box(groups, which, write):
    for n, boxes in enumerate(groups):
        first = 2 * n

        @pl.when((which >= first) & (which < first + 2))
        def _():
            def block(c, carry):
                write(c, boxes[which - first, :, columns(c)])
                return carry

            lax.fori_loop(0, COLS, block, 0, unroll=8)


def solve_pair(groups, first, second, delta, within, buffer, still, shifted, basis, image):
    def to_buffer(c, block):
        buffer[c + FRONT, pl.ds(ROOM, BOX), :] = block

    def to_still(c, block):
        still[c] = block

    load_box(groups, first, to_buffer)
    load_box(groups, second, to_still)
    read = shift_reader(buffer, *delta)
    diagonal, coupling = [], []
    norm_before = None
    for k in range(ITERS):
        field = basis.at[k]

        def value_of(c):
            if k == 0:
                moved = read(c)
                shifted[c] = moved
                return still[c] * moved
            fresh = image[c] - diagonal[k - 1] * basis[k - 1, c + 1, pl.ds(8, BOX), :]
            if k > 1:
                fresh = fresh - coupling[k - 1] * basis[k - 2, c + 1, pl.ds(8, BOX), :]
            return fresh

        def group(start, carry, final):
            norm, cross = carry
            center = field[start + 1, pl.ds(8, BOX), :]
            values = [center]
            for u in range(1, GROUP + 1):
                if final and u == GROUP:
                    values.append(jnp.zeros_like(center))
                    continue
                fresh = value_of(start + u)
                field[start + u + 1, pl.ds(8, BOX), :] = fresh
                norm = norm + fold(fresh * fresh)
                values.append(fresh)
            for u in range(GROUP):
                result = beside(field, start + u, values[u], values[u + 1], within)
                if k < ITERS - 1:
                    image[start + u] = result
                cross = cross + fold(values[u] * result)
            return norm, cross

        opening = value_of(0)
        field[1, pl.ds(8, BOX), :] = opening
        carry = (fold(opening * opening), jnp.zeros((8, LANES), jnp.float32))
        carry = lax.fori_loop(0, COLS // GROUP - 1, lambda m, held: group(m * GROUP, held, False), carry)
        norm, cross = group(COLS - GROUP, carry, True)
        norm = total(norm)
        diagonal.append(total(cross) / norm)
        coupling.append(norm / norm_before if k > 0 else None)
        norm_before = norm
    pivots = [SCREEN - diagonal[0]]
    rights = [jnp.ones_like(pivots[0])]
    for k in range(1, ITERS):
        pivots.append(SCREEN - diagonal[k] - coupling[k] / pivots[k - 1])
        rights.append(rights[k - 1] / pivots[k - 1])
    weights = [None] * ITERS
    weights[ITERS - 1] = rights[ITERS - 1] / pivots[ITERS - 1]
    for k in range(ITERS - 2, -1, -1):
        weights[k] = (rights[k] + coupling[k + 1] * weights[k + 1]) / pivots[k]
    return weights


def run_pair(groups, first, second, delta, to_second, to_first, within, forces, *scratch):
    buffer, still, shifted, basis, image = scratch
    weights = solve_pair(groups, first, second, delta, within, *scratch)

    def finish(c, carry):
        potential = weights[0] * basis[0, c + 1, pl.ds(8, BOX), :]
        for k in range(1, ITERS):
            potential = potential + weights[k] * basis[k, c + 1, pl.ds(8, BOX), :]
        image[c] = potential
        buffer[c + FRONT, pl.ds(ROOM, BOX), :] = potential * still[c]
        return carry

    lax.fori_loop(0, COLS, finish, 0, unroll=4)

    @pl.when(to_second)
    def _():
        def deposit(c, carry):
            forces[second, c] = forces[second, c] + image[c] * shifted[c]
            return carry

        lax.fori_loop(0, COLS, deposit, 0, unroll=4)

    @pl.when(to_first)
    def _():
        read = shift_reader(buffer, -delta[0], -delta[1], -delta[2])

        def deposit(c, carry):
            forces[first, c] = forces[first, c] + read(c)
            return carry

        lax.fori_loop(0, COLS, deposit, 0, unroll=8)


def pairs_kernel(kinds, *refs):
    begun, ending = kinds != ("own",), "far" in kinds
    lists, refs = refs[: len(kinds)], refs[len(kinds) :]
    offsets, own, elsewhere, within, *refs = refs
    if begun:
        tally, forces_in, *refs = refs
    if ending:
        *parts, forces = refs[:5]
    else:
        forces, tally_out = refs[:2]
    other, arrival, table, *scratch = refs[-8:]
    buffer, basis = scratch[0], scratch[3]
    group, mine = place()
    near, far = neighbours(group)
    neighbour = far if ending else near
    copy = pltpu.make_async_copy(elsewhere, other, arrival)
    copy.start()

    def clear(c, carry):
        buffer[c] = jnp.zeros((BOX + 2 * ROOM, LANES), jnp.float32)
        return carry

    lax.fori_loop(0, COLS + 2 * FRONT, clear, 0, unroll=4)
    nothing = jnp.zeros((BOX + 16, LANES), jnp.float32)
    for k in range(ITERS):
        basis[k, 0] = nothing

        def clear_ends(c, carry):
            basis[k, c + 1, pl.ds(0, 8), :] = jnp.zeros((8, LANES), jnp.float32)
            basis[k, c + 1, pl.ds(BOX + 8, 8), :] = jnp.zeros((8, LANES), jnp.float32)
            return carry

        lax.fori_loop(0, COLS, clear_ends, 0, unroll=4)

    def open_forces(c, carry):
        for k in range(2):
            forces[k, c] = forces_in[k, c] if begun else jnp.zeros((BOX, LANES), jnp.float32)
        return carry

    lax.fori_loop(0, COLS, open_forces, 0, unroll=2)

    def scan_list(kind, slots, carry):
        def scan(row, carry):
            count, found = carry
            base = ((row >> 2) ^ mine) * 12 + (row & 3) * 3
            first, second, live = slots[base], slots[base + 1], slots[base + 2]
            second_group = second >> 1
            wanted = second_group == (neighbour if kind == "own" else group)
            if kind == "own" and not ending:
                wanted = wanted | (second_group == group)
            taken = (live > 0) & wanted
            table[3 * found] = int(kind == "own")
            table[3 * found + 1] = first
            table[3 * found + 2] = second
            found = found + (taken & ((count & 3) == mine)).astype(jnp.int32)
            return count + taken.astype(jnp.int32), found

        return lax.fori_loop(0, 16, scan, carry, unroll=4)

    carry = (tally[0] if begun else jnp.int32(0), jnp.int32(0))
    for kind, slots in zip(kinds, lists):
        carry = scan_list(kind, slots, carry)
    count, found = carry
    copy.wait()

    def pair(m, carry):
        home, first, second = table[3 * m], table[3 * m + 1], table[3 * m + 2]
        delta = [offsets[first * 3 + axis] - offsets[second * 3 + axis] for axis in range(3)]

        def box_of(orbital):
            return jnp.where((orbital >> 1) == group, orbital - 2 * group, 2 + orbital - 2 * neighbour)

        run_pair(
            (own, other), box_of(first), box_of(second), delta, (second >> 1) == group, home > 0, within, forces, *scratch
        )
        return carry

    lax.fori_loop(0, found, pair, 0)
    if not ending:
        tally_out[0] = count
        return
    for k, side in enumerate((1, 3)):
        for n, who in enumerate((mine ^ side, mine)):
            for half, quarter in enumerate((who, who ^ (4 - side))):
                for c in range(QUARTER):
                    parts[2 * k + n][half * QUARTER + c] = forces[k, quarter * QUARTER + c]


def within_block():
    lane = np.arange(LANES)
    gap = np.abs(lane[:, None] - lane[None, :])
    same_row = lane[:, None] // BOX == lane[None, :] // BOX
    once = ((gap == 1) & same_row) | (gap == BOX)
    return jnp.asarray(np.concatenate([once, once]), jnp.bfloat16)


def stage_kernel(boxes, out):
    pltpu.sync_copy(boxes, out)


def stage(boxes):
    return pl.pallas_call(
        stage_kernel,
        out_shape=jax.ShapeDtypeStruct(boxes.shape, boxes.dtype),
        in_specs=[HBM],
        out_specs=VMEM,
        compiler_params=pltpu.CompilerParams(vmem_limit_bytes=SMALL_VMEM),
        cost_estimate=pl.CostEstimate(flops=1_000_000, bytes_accessed=4 << 20, transcendentals=0),
        name="stage",
    )(boxes)


def run_pairs(lists, offsets, own, other, before=()):
    kinds = tuple(lists)
    operands = [*lists.values(), offsets, own, other, within_block(), *before]
    in_specs = [SMEM] * (len(kinds) + 1) + [VMEM, HBM, VMEM] + [SMEM, VMEM][: len(before)]
    whole = (2, COLS, BOX, LANES)
    scratch = [
        pltpu.VMEM((2, BOX, BOX * BOX), jnp.float32),
        pltpu.SemaphoreType.DMA,
        pltpu.SMEM((3 * 64,), jnp.int32),
        pltpu.VMEM((COLS + 2 * FRONT, BOX + 2 * ROOM, LANES), jnp.float32),
        pltpu.VMEM((COLS, BOX, LANES), jnp.float32),
        pltpu.VMEM((COLS, BOX, LANES), jnp.float32),
        pltpu.VMEM((ITERS, COLS + 1, BOX + 16, LANES), jnp.float32),
        pltpu.VMEM((COLS, BOX, LANES), jnp.float32),
    ]
    if "far" in kinds:
        out_shape = [jax.ShapeDtypeStruct((2 * QUARTER, BOX, LANES), jnp.float32)] * 4
        out_specs = [VMEM] * 4
        scratch = [pltpu.VMEM(whole, jnp.float32)] + scratch
    else:
        out_shape = [jax.ShapeDtypeStruct(whole, jnp.float32), jax.ShapeDtypeStruct((1,), jnp.int32)]
        out_specs = [VMEM, SMEM]
    return pl.pallas_call(
        functools.partial(pairs_kernel, kinds),
        out_shape=out_shape,
        in_specs=in_specs,
        out_specs=out_specs,
        scratch_shapes=scratch,
        compiler_params=pltpu.CompilerParams(vmem_limit_bytes=PAIRS_VMEM),
        cost_estimate=pl.CostEstimate(flops=100_000_000, bytes_accessed=8 << 20, transcendentals=0),
    )(*operands)


def settle_kernel(offsets, *refs):
    parts, sums, pieces, tall = refs[:6], refs[6:8], refs[8:13], refs[13]
    group, _ = place()
    for k in range(2):
        kept, once, twice = parts[3 * k : 3 * k + 3]
        tall[:, pl.ds(0, SLAB), :] = jnp.zeros((QUARTER, SLAB, LANES), jnp.float32)
        tall[:, pl.ds(SLAB + BOX, SLAB), :] = jnp.zeros((QUARTER, SLAB, LANES), jnp.float32)
        for c in range(QUARTER):
            value = (kept[c] + once[c]) + twice[c]
            sums[k][c] = value
            tall[c, pl.ds(SLAB, BOX), :] = value
        depth = offsets[(2 * group + k) * 3] - group * SLAB
        for t in range(SLABS):
            for c in range(QUARTER):
                pieces[t][k, c] = tall[c, pl.ds(SLAB * (t + 1) - depth, SLAB), :]


def settle(offsets, parts):
    quarter = jax.ShapeDtypeStruct((QUARTER, BOX, LANES), jnp.float32)
    piece = jax.ShapeDtypeStruct((2, QUARTER, SLAB, LANES), jnp.float32)
    return pl.pallas_call(
        settle_kernel,
        out_shape=[quarter] * 2 + [piece] * SLABS,
        in_specs=[SMEM] + [VMEM] * 6,
        out_specs=[VMEM] * (2 + SLABS),
        scratch_shapes=[pltpu.VMEM((QUARTER, BOX + 2 * SLAB, LANES), jnp.float32)],
        cost_estimate=pl.CostEstimate(flops=4_000_000, bytes_accessed=4 << 20, transcendentals=0),
        compiler_params=pltpu.CompilerParams(vmem_limit_bytes=SMALL_VMEM),
        name="settle",
    )(offsets, *parts)


def deposit_kernel(offsets, *refs):
    pieces, outs, span = refs[:SLABS], refs[SLABS : SLABS + 2], refs[-1]
    group, _ = place()
    lanes = lax.broadcasted_iota(jnp.int32, (SLAB, LANES), 1)
    span[...] = jnp.zeros_like(span)
    for t in range(SLABS):
        owner = (group + lax.axis_size("orb") - t) % lax.axis_size("orb")

        def lay(k, carry):
            at = (2 * owner + k) * 3
            base = offsets[at + 1] * WIDE + offsets[at + 2]
            for c in range(QUARTER):
                value = pieces[t][k, c]
                for row in range(2):
                    start = base + (2 * c + row) * WIDE - row * BOX
                    tile, turn = start >> 7, start & (LANES - 1)
                    kept = (lanes < BOX) if row == 0 else (lanes >= BOX)
                    turned = pltpu.roll(jnp.where(kept, value, 0.0), turn, 1)
                    here = pl.ds(pl.multiple_of(tile * LANES, LANES), LANES)
                    there = pl.ds(pl.multiple_of(tile * LANES + LANES, LANES), LANES)
                    span[:, here] = span[:, here] + jnp.where(lanes >= turn, turned, 0.0)
                    span[:, there] = span[:, there] + jnp.where(lanes < turn, turned, 0.0)
            return carry

        lax.fori_loop(0, 2, lay, 0)
    for half in range(2):
        outs[half][...] = span[pl.ds(8 * half, 8), pl.ds(0, SPAN)]


def deposit(offsets, pieces):
    half = jax.ShapeDtypeStruct((SLAB // 2, SPAN), jnp.float32)
    return pl.pallas_call(
        deposit_kernel,
        out_shape=[half] * 2,
        in_specs=[SMEM] + [VMEM] * SLABS,
        out_specs=[VMEM] * 2,
        scratch_shapes=[pltpu.VMEM((SLAB, SPAN + 4 * LANES), jnp.float32)],
        cost_estimate=pl.CostEstimate(flops=8_000_000, bytes_accessed=2 << 20, transcendentals=0),
        compiler_params=pltpu.CompilerParams(vmem_limit_bytes=SMALL_VMEM),
        name="deposit",
    )(offsets, *pieces)


def quarters_of(mine):
    return mine, mine ^ 1, mine ^ 3, mine ^ 2


def merge_kernel(*refs):
    spans, out = refs[:8], refs[8]
    _, mine = place()
    out[...] = jnp.zeros_like(out)
    for n, quarter in enumerate(quarters_of(mine)):
        where = pl.ds(pl.multiple_of(quarter * (WIDE * BOX // 4), LANES), SPAN)
        for half in range(2):
            rows = pl.ds(8 * half, 8)
            out[rows, where] = out[rows, where] + spans[2 * n + half][...]


def merge(spans):
    return pl.pallas_call(
        merge_kernel,
        out_shape=jax.ShapeDtypeStruct((SLAB, WIDE * WIDE), jnp.float32),
        in_specs=[VMEM] * 8,
        out_specs=VMEM,
        cost_estimate=pl.CostEstimate(flops=1_000_000, bytes_accessed=2 << 20, transcendentals=0),
        compiler_params=pltpu.CompilerParams(vmem_limit_bytes=SMALL_VMEM),
        name="merge",
    )(*spans)


def assemble_kernel(*refs):
    parts, out = refs[:8], refs[8]
    _, mine = place()
    for n, quarter in enumerate(quarters_of(mine)):
        for k in range(2):
            for c in range(QUARTER):
                where = pl.ds(pl.multiple_of((quarter * QUARTER + c) * LANES, LANES), LANES)
                out[k, :, where] = parts[2 * n + k][c]


def assemble(parts):
    return pl.pallas_call(
        assemble_kernel,
        out_shape=jax.ShapeDtypeStruct((2, BOX, BOX * BOX), jnp.float32),
        in_specs=[VMEM] * 8,
        out_specs=VMEM,
        cost_estimate=pl.CostEstimate(flops=1_000_000, bytes_accessed=4 << 20, transcendentals=0),
        compiler_params=pltpu.CompilerParams(vmem_limit_bytes=SMALL_VMEM),
        name="assemble",
    )(*parts)


def across(block, side):
    return lax.ppermute(block, "rep", [(i, i ^ side) for i in range(lax.axis_size("rep"))])


def gather_pair(first, second):
    first_three, second_one = across(first, 3), across(second, 1)
    first_one, second_three = across(first, 1), across(second, 3)
    first_two = across(first_three, 1)
    second_two = across(second_one, 3)
    return [first, second, first_one, second_one, first_three, second_three, first_two, second_two]


def shards(orbitals, pair_list, box_offsets):
    groups = lax.axis_size("orb")
    to_near = [(g, g ^ 1) for g in range(groups)]
    to_far = [(g, neighbours(g)[1]) for g in range(groups) if 0 <= neighbours(g)[1] < groups]
    slots = pair_list.reshape(-1)
    known = jnp.concatenate([slots] + [across(slots, side) for side in (1, 2, 3)])
    near = lax.ppermute(orbitals, "orb", to_near)
    far = lax.ppermute(orbitals, "orb", to_far)
    near_list = lax.ppermute(known, "orb", to_near)
    far_list = lax.ppermute(known, "orb", to_far)
    offsets = box_offsets.reshape(-1)
    own = stage(orbitals)
    shared, tally = run_pairs({"own": known}, offsets, own, near)
    shared, tally = run_pairs({"near": near_list}, offsets, own, near, (tally, shared))
    parts = run_pairs({"own": known, "far": far_list}, offsets, own, far, (tally, shared))
    sent_zero, kept_zero, sent_one, kept_one = parts
    got_zero, got_one = across(sent_zero, 1), across(sent_one, 3)
    last_zero = across(kept_zero[QUARTER:] + got_zero[QUARTER:], 3)
    last_one = across(kept_one[QUARTER:] + got_one[QUARTER:], 1)
    settled = settle(offsets, (kept_zero, got_zero, last_zero, kept_one, got_one, last_one))
    pieces = [settled[2]]
    for later in range(1, SLABS):
        route = [(i, (i + later) % groups) for i in range(groups)]
        pieces.append(lax.ppermute(settled[2 + later], "orb", route))
    gathered = gather_pair(settled[0], settled[1])
    forces = assemble(gathered)
    spans = deposit(offsets, pieces)
    gathered = gather_pair(*spans)
    slab = merge(gathered)
    return (forces, slab)


def solution(mesh):
    in_specs = (P("orb", None, None), P(("orb", "rep"), None), P())
    out_specs = (P("orb", None, None), P("orb", None))
    return jax.shard_map(shards, mesh=mesh, in_specs=in_specs, out_specs=out_specs, check_vma=False)
```
